8 devices in a mesh: row: 2 (over z, y), col: 4 (over x, core).
Axes of the slice: x: 2, y: 2, z: 1, core: 2. Of those that a mesh axis runs over, the one named last changes fastest.
Arguments:
- v_panels: float32 [4096, 4096], P('row', 'col')
- t_factors: float32 [64, 64, 64], P('col')
- z_vectors: float32 [4096, 2048], P(None, ('col', 'row'))
Outputs:
- output: float32 [4096, 2048], P('row', 'col')
All inputs are finite; a program needn't handle non-finite values.
Results may differ from the reference program's by a relative error of at most 0.001.
Values sent between devices are 32-bit elements.
A program may use at most 1 GiB of HBM per device.

```python
import jax
import jax.numpy as jnp
from jax import lax

MAT_ORDER = 4096
PANEL_WIDTH = 64
ROW_DEVS = 2
COL_DEVS = 4
COLS_DEV = 256
NUM_PANELS = MAT_ORDER // PANEL_WIDTH
NUM_COLS = COLS_DEV * ROW_DEVS * COL_DEVS
HIGHEST = lax.Precision.HIGHEST


def compact_factors(panels):
    gram_mat = jnp.einsum('nja,njc->jac', panels, panels, precision=HIGHEST)
    diag_half = 0.5 * gram_mat * jnp.eye(PANEL_WIDTH, dtype=jnp.float32)
    upper_mat = jnp.triu(gram_mat, 1) + diag_half
    return jnp.triu(jnp.linalg.inv(upper_mat))


def to_stored(v_log):
    rows_perm = v_log.reshape(NUM_PANELS // ROW_DEVS, ROW_DEVS, PANEL_WIDTH, MAT_ORDER)
    rows_perm = rows_perm.transpose(1, 0, 2, 3).reshape(MAT_ORDER, NUM_PANELS // COL_DEVS, COL_DEVS, PANEL_WIDTH)
    return rows_perm.transpose(0, 2, 1, 3).reshape(MAT_ORDER, MAT_ORDER)


def setup_inputs(seed: int = 0) -> dict:
    root_key = jax.random.key(seed)
    key_v, key_z = jax.random.split(root_key)
    below_diag = jax.random.normal(key_v, (MAT_ORDER, MAT_ORDER), jnp.float32)
    v_log = jnp.tril(below_diag, -1) + jnp.eye(MAT_ORDER, dtype=jnp.float32)
    t_log = compact_factors(v_log.reshape(MAT_ORDER, NUM_PANELS, PANEL_WIDTH))
    t_st = t_log.reshape(NUM_PANELS // COL_DEVS, COL_DEVS, PANEL_WIDTH, PANEL_WIDTH)
    t_st = t_st.transpose(1, 0, 2, 3).reshape(NUM_PANELS, PANEL_WIDTH, PANEL_WIDTH)
    z_draw = jax.random.normal(key_z, (MAT_ORDER, NUM_COLS), jnp.float32)
    return {'v_panels': to_stored(v_log), 't_factors': t_st, 'z_vectors': z_draw}


def reference(v_panels, t_factors, z_vectors):
    panels = v_panels.reshape(MAT_ORDER, COL_DEVS, NUM_PANELS // COL_DEVS, PANEL_WIDTH)
    panels = panels.transpose(2, 1, 0, 3).reshape(NUM_PANELS, MAT_ORDER, PANEL_WIDTH)
    factors = t_factors.reshape(COL_DEVS, NUM_PANELS // COL_DEVS, PANEL_WIDTH, PANEL_WIDTH)
    factors = factors.transpose(1, 0, 2, 3).reshape(NUM_PANELS, PANEL_WIDTH, PANEL_WIDTH)

    def apply_panel(x_cur, panel_item):
        v_j, t_j = panel_item
        w_mat = jnp.dot(v_j.T, x_cur, precision=HIGHEST, preferred_element_type=jnp.float32)
        y_mat = jnp.dot(t_j, w_mat, precision=HIGHEST, preferred_element_type=jnp.float32)
        x_new = x_cur - jnp.dot(v_j, y_mat, precision=HIGHEST, preferred_element_type=jnp.float32)
        return x_new, None

    return lax.scan(apply_panel, z_vectors, (panels, factors), reverse=True)[0]
```

```python
import jax
import jax.numpy as jnp
from jax import lax
from jax.experimental import pallas as pl
from jax.experimental.pallas import tpu as pltpu
from jax.sharding import PartitionSpec as P

F32 = jnp.float32
BF16 = jnp.bfloat16
MESH = pl.DeviceIdType.MESH
PW = 64
RB = 256
GROUPS = 8
BLOCKS = GROUPS * (GROUPS + 1) // 2
HALF = RB // 2
AHEAD_W = 3
OWN_LEAD = 2
COLS = 256
ROWS = 2048
GW = GROUPS * PW
HW = GW // 2
VMEM_LIMIT = 66 * 10**6


def split3(x):
    a = x.astype(BF16)
    r = x - a.astype(F32)
    b = r.astype(BF16)
    c = (r - b.astype(F32)).astype(BF16)
    return a, b, c


def dot6(lhs, rhs):
    a1, a2, a3 = lhs
    b1, b2, b3 = rhs

    def mm(p, q):
        return jnp.dot(p, q, preferred_element_type=F32)

    return ((mm(a3, b1) + mm(a1, b3)) + mm(a2, b2)) + (mm(a2, b1) + mm(a1, b2)) + mm(a1, b1)


def dot_f32(a, b):
    return dot6(split3(a), split3(b))


def kernel(v_hbm, t_hbm, z_hbm, out_hbm, v_buf, t_buf, x_buf, w0, w1, g00, g01, g11, y_buf,
           loc_sem, t_send, t_recv, send, recv, c_send, c_recv, io_sem):
    row = lax.axis_index('row')
    col = lax.axis_index('col')
    orow = 1 - row
    xcol = lax.rem(col + 2, 4)
    pcol = col + 1 - 2 * lax.rem(col, 2)
    x_dev, y_dev, p_dev = (row, xcol), (orow, col), (row, pcol)
    me = row * 4 + col
    xs = row * 4 + xcol
    ys = orow * 4 + col
    ds = orow * 4 + xcol

    def vmem(slot, blk, off=0, size=RB):
        return v_buf.at[slot, pl.ds(pl.multiple_of(blk * RB + off, HALF), size), :]

    def rcopy(slot, blk, kind, dev, off=0, size=RB):
        return pltpu.make_async_remote_copy(
            src_ref=vmem(slot, blk, off, size), dst_ref=vmem(slot, blk, off, size),
            send_sem=send.at[kind, blk], recv_sem=recv.at[kind, blk], device_id=dev, device_id_type=MESH)

    OX, OY, OP, FX, FY, PX, PY, PD = range(8)

    def own(blk):
        return (rcopy(me, blk, OX, x_dev), rcopy(me, blk, OY, y_dev), rcopy(me, blk, OP, p_dev))

    def fwd(blk):
        return (rcopy(xs, blk, FY, y_dev, 0, HALF), rcopy(ys, blk, FX, x_dev, HALF, HALF),
                rcopy(xs, blk, PX, p_dev), rcopy(ys, blk, PY, p_dev))

    def diag(blk):
        return rcopy(ds, blk, PD, p_dev)

    def t_copy(slot, kind, dev):
        return pltpu.make_async_remote_copy(
            src_ref=t_buf.at[slot], dst_ref=t_buf.at[slot], send_sem=t_send.at[kind], recv_sem=t_recv.at[kind],
            device_id=dev, device_id_type=MESH)

    def local_v(n):
        k = GROUPS - n
        o = n * (n - 1) // 2
        return pltpu.make_async_copy(
            v_hbm.at[pl.ds(RB * k, RB * n), pl.ds(2 * PW * k, 2 * PW)],
            v_buf.at[me, pl.ds(RB * o, RB * n), :], loc_sem.at[n - 1])

    for n in range(1, GROUPS + 1):
        local_v(n).start()
    t_in = pltpu.make_async_copy(t_hbm, t_buf.at[col], io_sem.at[0])
    t_in.start()
    z_in = pltpu.make_async_copy(z_hbm, x_buf, io_sem.at[1])
    z_in.start()

    barrier = pltpu.get_barrier_semaphore()
    for dev in (x_dev, y_dev, p_dev):
        pl.semaphore_signal(barrier, inc=1, device_id=dev, device_id_type=MESH)
    pl.semaphore_wait(barrier, 3)

    for n in range(1, GROUPS + 1):
        local_v(n).wait()
        if n == 2:
            for b in range(OWN_LEAD):
                for c in own(b):
                    c.start()
            t_in.wait()
            t_copy(col, 0, x_dev).start()
            t_copy(col, 1, p_dev).start()
    z_in.wait()

    def pump(blk, _):
        rcopy(xs, blk, OX, x_dev).wait_recv()
        rcopy(ys, blk, OY, y_dev).wait_recv()
        for c in fwd(blk):
            c.start()

        @pl.when(blk + OWN_LEAD < BLOCKS)
        def _():
            for c in own(blk + OWN_LEAD):
                c.start()
        return 0

    def pump_to(done, target):
        target = jnp.maximum(done, jnp.minimum(target, BLOCKS))
        lax.fori_loop(done, target, pump, 0)
        return target

    def take_diag(blk):
        rcopy(ds, blk, FY, y_dev, 0, HALF).wait_recv()
        rcopy(ds, blk, FX, x_dev, HALF, HALF).wait_recv()
        diag(blk).start()

    def need(blk):
        rcopy(me, blk, OP, p_dev).wait_recv()
        rcopy(me, blk, PX, p_dev).wait_recv()
        rcopy(me, blk, PY, p_dev).wait_recv()
        rcopy(me, blk, PD, p_dev).wait_recv()

    lane = lax.broadcasted_iota(jnp.int32, (RB, 128), 1)

    def halves(dd, blk):
        r = pl.ds(pl.multiple_of(blk * RB, RB), RB)
        tiles = [v_buf[dd * 4 + e, r, :] for e in range(4)]
        rolled = [pltpu.roll(t, PW, 1) for t in tiles]
        low = [jnp.where(lane < PW, tiles[e], rolled[e + 1]) for e in (0, 2)]
        high = [jnp.where(lane < PW, rolled[e], tiles[e + 1]) for e in (0, 2)]
        return jnp.concatenate(low, axis=1), jnp.concatenate(high, axis=1)

    ri = lax.broadcasted_iota(jnp.int32, (HW, HW), 0) // PW
    ci = lax.broadcasted_iota(jnp.int32, (HW, HW), 1) // PW
    near = jnp.logical_and(ri // 2 == ci // 2, ri < ci)
    far = ri // 2 < ci // 2

    def block_t(k, par):
        rows = []
        for e in range(4):
            t = t_buf[e, pl.ds(pl.multiple_of(k * PW, PW), PW), :]
            r = pltpu.roll(t, PW, 1)
            src = t if par == e % 2 else r
            keep = lax.broadcasted_iota(jnp.int32, (PW, 128), 1) // PW == e % 2
            tile = jnp.where(keep, src, 0.0)
            zero = jnp.zeros((PW, 128), F32)
            rows.append(jnp.concatenate([tile, zero] if e < 2 else [zero, tile], axis=1))
        return jnp.concatenate(rows, axis=0)

    def merge(t, g):
        t = t - dot_f32(t, dot_f32(jnp.where(near, g, 0.0), t))
        return t - dot_f32(t, dot_f32(jnp.where(far, g, 0.0), t))

    def group(step, carry):
        pumped, diag_done = carry
        n = step + 1
        k = GROUPS - n
        first = n * step // 2
        w0[...] = jnp.zeros_like(w0)
        w1[...] = jnp.zeros_like(w1)
        g00[...] = jnp.zeros_like(g00)
        g01[...] = jnp.zeros_like(g01)
        g11[...] = jnp.zeros_like(g11)

        def gather_step(i, carry):
            pumped, diag_done = carry
            blk = first + i
            pumped = pump_to(pumped, blk + AHEAD_W)

            def dg(b, _):
                take_diag(b)
                return 0
            diag_to = jnp.minimum(blk + 2, BLOCKS)
            lax.fori_loop(diag_done, diag_to, dg, 0)
            need(blk)
            r = pl.ds(pl.multiple_of((k + i) * RB, RB), RB)
            parts = [halves(dd, blk) for dd in range(2)]
            v0 = split3(jnp.concatenate([p[0] for p in parts], axis=0))
            v1 = split3(jnp.concatenate([p[1] for p in parts], axis=0))
            x = split3(jnp.concatenate([x_buf[0, r, :], x_buf[1, r, :]], axis=0))
            t0 = [t.T for t in v0]
            t1 = [t.T for t in v1]
            w0[...] += dot6(t0, x)
            w1[...] += dot6(t1, x)
            g00[...] += dot6(t0, v0)
            g01[...] += dot6(t0, v1)
            g11[...] += dot6(t1, v1)
            return pumped, diag_to

        pumped, diag_done = lax.fori_loop(0, n, gather_step, (pumped, diag_done))

        @pl.when(step == 0)
        def _():
            t_copy(xcol, 0, x_dev).wait_recv()
            t_copy(xcol, 2, p_dev).start()
            t_copy(pcol, 1, p_dev).wait_recv()
            t_copy(lax.rem(pcol + 2, 4), 2, p_dev).wait_recv()

        ta = merge(block_t(k, 0), g00[...])
        tb = merge(block_t(k, 1), g11[...])
        y1 = dot_f32(tb, w1[...])
        y0 = dot_f32(ta, w0[...] - dot_f32(g01[...], y1))
        for e in range(4):
            y_buf[e * 128:e * 128 + PW, :] = y0[e * PW:(e + 1) * PW]
            y_buf[e * 128 + PW:(e + 1) * 128, :] = y1[e * PW:(e + 1) * PW]

        def update_step(i, pumped):
            blk = first + i
            pumped = pump_to(pumped, first + n - 1 + AHEAD_W + (i + 1) // 2)
            rv = pl.ds(pl.multiple_of(blk * RB, RB), RB)
            rx = pl.ds(pl.multiple_of((k + i) * RB, RB), RB)
            v = jnp.concatenate(
                [jnp.concatenate([v_buf[dd * 4 + e, rv, :] for e in range(4)], axis=1) for dd in range(2)], axis=0)
            delta = dot6(split3(v), split3(y_buf[...]))
            x_buf[0, rx, :] = x_buf[0, rx, :] - delta[:RB]
            x_buf[1, rx, :] = x_buf[1, rx, :] - delta[RB:]

            @pl.when(jnp.logical_and(k == 0, i > 0))
            def _():
                give(i - 1).start()
            return pumped

        pumped = lax.fori_loop(0, n, update_step, pumped)
        return pumped, diag_done

    def give(i):
        r = pl.ds(pl.multiple_of(i * RB, RB), RB)
        return pltpu.make_async_remote_copy(
            src_ref=x_buf.at[orow, r, :],
            dst_ref=out_hbm.at[r, pl.ds(pl.multiple_of(row * COLS, COLS), COLS)],
            send_sem=c_send.at[i], recv_sem=c_recv.at[i], device_id=y_dev, device_id_type=MESH)

    lax.fori_loop(0, GROUPS, group, (0, 0))

    def drain(blk, _):
        for c in own(blk):
            c.wait_send()
        for c in fwd(blk):
            c.wait_send()
        diag(blk).wait_send()
        return 0
    lax.fori_loop(0, BLOCKS, drain, 0)
    t_copy(col, 0, x_dev).wait_send()
    t_copy(col, 1, p_dev).wait_send()
    t_copy(xcol, 2, p_dev).wait_send()

    give(GROUPS - 1).start()
    keep = pltpu.make_async_copy(
        x_buf.at[row], out_hbm.at[:, pl.ds(pl.multiple_of(row * COLS, COLS), COLS)], io_sem.at[2])
    keep.start()
    keep.wait()

    def drain_c(i, _):
        give(i).wait()
        return 0
    lax.fori_loop(0, GROUPS, drain_c, 0)


def solution(mesh):
    def local_apply(v_loc, t_loc, z_loc):
        t_pk = t_loc.reshape(GROUPS, 2, PW, PW).transpose(0, 2, 1, 3).reshape(GROUPS * PW, 2 * PW)
        z_pk = z_loc.reshape(2, ROWS, COLS)
        any_spec = pl.BlockSpec(memory_space=pl.ANY)
        return pl.pallas_call(
            kernel,
            out_shape=jax.ShapeDtypeStruct((ROWS, 2 * COLS), F32),
            in_specs=[any_spec] * 3,
            out_specs=any_spec,
            scratch_shapes=[
                pltpu.VMEM((8, BLOCKS * RB, 128), F32),
                pltpu.VMEM((4, GROUPS * PW, 128), F32),
                pltpu.VMEM((2, ROWS, COLS), F32),
                pltpu.VMEM((HW, COLS), F32),
                pltpu.VMEM((HW, COLS), F32),
                pltpu.VMEM((HW, HW), F32),
                pltpu.VMEM((HW, HW), F32),
                pltpu.VMEM((HW, HW), F32),
                pltpu.VMEM((GW, COLS), F32),
                pltpu.SemaphoreType.DMA((GROUPS,)),
                pltpu.SemaphoreType.DMA((3,)),
                pltpu.SemaphoreType.DMA((3,)),
                pltpu.SemaphoreType.DMA((8, BLOCKS)),
                pltpu.SemaphoreType.DMA((8, BLOCKS)),
                pltpu.SemaphoreType.DMA((GROUPS,)),
                pltpu.SemaphoreType.DMA((GROUPS,)),
                pltpu.SemaphoreType.DMA((3,)),
            ],
            compiler_params=pltpu.CompilerParams(
                collective_id=0, has_side_effects=True, vmem_limit_bytes=VMEM_LIMIT),
            name='panels',
        )(v_loc, t_pk, z_pk)

    return jax.shard_map(local_apply, mesh=mesh,
                         in_specs=(P('row', 'col'), P('col', None, None), P(None, ('col', 'row'))),
                         out_specs=P('row', 'col'), check_vma=False)
```

```python
import jax
import jax.numpy as jnp
from jax import lax
from jax.experimental import pallas as pl
from jax.experimental.pallas import tpu as pltpu
from jax.sharding import PartitionSpec as P

F32 = jnp.float32
BF16 = jnp.bfloat16
MESH = pl.DeviceIdType.MESH
PW = 64
RB = 256
GROUPS = 8
BLOCKS = GROUPS * (GROUPS + 1) // 2
HALF = RB // 2
AHEAD_W = 5
OWN_LEAD = 4
COLS = 256
ROWS = 2048
GW = GROUPS * PW
HW = GW // 2
VMEM_LIMIT = 66 * 10**6


def split3(x):
    a = x.astype(BF16)
    r = x - a.astype(F32)
    b = r.astype(BF16)
    c = (r - b.astype(F32)).astype(BF16)
    return a, b, c


def dot6(lhs, rhs):
    a1, a2, a3 = lhs
    b1, b2, b3 = rhs

    def mm(p, q):
        return jnp.dot(p, q, preferred_element_type=F32)

    return ((mm(a3, b1) + mm(a1, b3)) + mm(a2, b2)) + (mm(a2, b1) + mm(a1, b2)) + mm(a1, b1)


def dot_f32(a, b):
    return dot6(split3(a), split3(b))


def kernel(v_hbm, t_hbm, z_hbm, out_hbm, v_buf, t_buf, x_buf, w_buf, g_part, g_in, g_last, y_buf,
           loc_sem, t_send, t_recv, send, recv, g_send, g_recv, c_send, c_recv, io_sem):
    row = lax.axis_index('row')
    col = lax.axis_index('col')
    orow = 1 - row
    xcol = lax.rem(col + 2, 4)
    core = lax.rem(col, 2)
    pcol = col + 1 - 2 * core
    x_dev, y_dev, p_dev = (row, xcol), (orow, col), (row, pcol)
    me = row * 4 + col
    xs = row * 4 + xcol
    ys = orow * 4 + col
    ds = orow * 4 + xcol

    def vmem(slot, blk, off=0, size=RB):
        return v_buf.at[slot, pl.ds(pl.multiple_of(blk * RB + off, HALF), size), :]

    def rcopy(slot, blk, kind, dev, off=0, size=RB):
        return pltpu.make_async_remote_copy(
            src_ref=vmem(slot, blk, off, size), dst_ref=vmem(slot, blk, off, size),
            send_sem=send.at[kind, blk], recv_sem=recv.at[kind, blk], device_id=dev, device_id_type=MESH)

    OX, OY, OP, FX, FY, PX, PY, PD = range(8)

    def own(blk):
        return (rcopy(me, blk, OX, x_dev), rcopy(me, blk, OY, y_dev), rcopy(me, blk, OP, p_dev))

    def fwd(blk):
        return (rcopy(xs, blk, FY, y_dev, 0, HALF), rcopy(ys, blk, FX, x_dev, HALF, HALF),
                rcopy(xs, blk, PX, p_dev), rcopy(ys, blk, PY, p_dev))

    def diag(blk):
        return rcopy(ds, blk, PD, p_dev)

    def t_copy(slot, kind, dev):
        return pltpu.make_async_remote_copy(
            src_ref=t_buf.at[slot], dst_ref=t_buf.at[slot], send_sem=t_send.at[kind], recv_sem=t_recv.at[kind],
            device_id=dev, device_id_type=MESH)

    def local_v(n):
        k = GROUPS - n
        o = n * (n - 1) // 2
        return pltpu.make_async_copy(
            v_hbm.at[pl.ds(RB * k, RB * n), pl.ds(2 * PW * k, 2 * PW)],
            v_buf.at[me, pl.ds(RB * o, RB * n), :], loc_sem.at[n - 1])

    for n in range(1, GROUPS + 1):
        local_v(n).start()
    t_in = pltpu.make_async_copy(t_hbm, t_buf.at[col], io_sem.at[0])
    t_in.start()
    z_in = pltpu.make_async_copy(z_hbm, x_buf, io_sem.at[1])
    z_in.start()

    barrier = pltpu.get_barrier_semaphore()
    for dev in (x_dev, y_dev, p_dev):
        pl.semaphore_signal(barrier, inc=1, device_id=dev, device_id_type=MESH)
    pl.semaphore_wait(barrier, 3)

    for n in range(1, GROUPS + 1):
        local_v(n).wait()
        if n == 4:
            for b in range(OWN_LEAD):
                for c in own(b):
                    c.start()
            t_in.wait()
            t_copy(col, 0, x_dev).start()
            t_copy(col, 1, p_dev).start()
    z_in.wait()

    def pump(blk, _):
        rcopy(xs, blk, OX, x_dev).wait_recv()
        rcopy(ys, blk, OY, y_dev).wait_recv()
        for c in fwd(blk):
            c.start()

        @pl.when(blk + OWN_LEAD < BLOCKS)
        def _():
            for c in own(blk + OWN_LEAD):
                c.start()
        return 0

    def pump_to(done, target):
        target = jnp.maximum(done, jnp.minimum(target, BLOCKS))
        lax.fori_loop(done, target, pump, 0)
        return target

    def take_diag(blk):
        rcopy(ds, blk, FY, y_dev, 0, HALF).wait_recv()
        rcopy(ds, blk, FX, x_dev, HALF, HALF).wait_recv()
        diag(blk).start()

    def need(blk):
        rcopy(me, blk, OP, p_dev).wait_recv()
        rcopy(me, blk, PX, p_dev).wait_recv()
        rcopy(me, blk, PY, p_dev).wait_recv()
        rcopy(me, blk, PD, p_dev).wait_recv()

    def rows_of(blk, dds):
        r = pl.ds(pl.multiple_of(blk * RB, RB), RB)
        return jnp.concatenate(
            [jnp.concatenate([v_buf[dd * 4 + e, r, :] for e in range(4)], axis=1) for dd in dds], axis=0)

    def gram(cols, vals):
        first = [t[:HW] for t in cols]
        last = [t[HW:] for t in cols]
        vf = [v[:, :HW] for v in vals]
        vl = [v[:, HW:] for v in vals]
        return dot6(first, vf), dot6(first, vl), dot6(last, vl)

    lane = lax.broadcasted_iota(jnp.int32, (HW, 128), 1)
    lane_t = lax.broadcasted_iota(jnp.int32, (PW, 128), 1)
    zero_t = jnp.zeros((PW, 128), F32)

    def lanes_of(q, par):
        a, b = q[:, :128], q[:, 128:]
        if par == 0:
            return jnp.where(lane < PW, a, pltpu.roll(b, PW, 1))
        return jnp.where(lane < PW, pltpu.roll(a, PW, 1), b)

    def rows_par(q, par):
        return jnp.concatenate([q[par * PW:(par + 1) * PW], q[128 + par * PW:128 + (par + 1) * PW]], axis=0)

    def factors(k, par):
        tiles = []
        for e in range(4):
            t = t_buf[e, pl.ds(pl.multiple_of(k * PW, PW), PW), :]
            src = t if par == e % 2 else pltpu.roll(t, PW, 1)
            tiles.append(jnp.where(lane_t // PW == e % 2, src, 0.0))
        return tiles

    def diag256(tiles):
        return jnp.concatenate(
            [jnp.concatenate([t, zero_t] if e < 2 else [zero_t, t], axis=1) for e, t in enumerate(tiles)], axis=0)

    def merge(tiles, gaa, gab, gbb):
        whole = diag256(tiles)
        u = jnp.concatenate([jnp.where(lane_t < PW, 0.0, gaa[:PW]), jnp.where(lane_t < PW, 0.0, gbb[:PW])], axis=1)
        c = dot_f32(u, whole)
        rhs = jnp.concatenate([
            jnp.concatenate([c[:, :128], zero_t], axis=1), jnp.zeros((PW, HW), F32),
            jnp.concatenate([zero_t, c[:, 128:]], axis=1), jnp.zeros((PW, HW), F32)], axis=0)
        lhs = jnp.concatenate([tiles[0] + tiles[1], tiles[2] + tiles[3]], axis=1)
        p = dot_f32(lhs, rhs)
        ta = jnp.concatenate([tiles[0] - p[:, :128], tiles[1]], axis=0)
        tb = jnp.concatenate([tiles[2] - p[:, 128:], tiles[3]], axis=0)
        tab = dot_f32(ta, dot_f32(gab, tb))
        return jnp.concatenate([
            jnp.concatenate([ta, -tab], axis=1), jnp.concatenate([jnp.zeros_like(tb), tb], axis=1)], axis=0)

    def g_copy(n):
        return pltpu.make_async_remote_copy(
            src_ref=g_part, dst_ref=g_in.at[lax.rem(n, 2)], send_sem=g_send, recv_sem=g_recv.at[lax.rem(n, 2)],
            device_id=p_dev, device_id_type=MESH)

    def group(step, carry):
        pumped, diag_done = carry
        n = step + 1
        k = GROUPS - n
        first = n * step // 2
        w_buf[...] = jnp.zeros_like(w_buf)

        @pl.when(n > 2)
        def _():
            g_copy(n - 1).wait_send()
        g_part[...] = jnp.zeros_like(g_part)

        def arrive(i, carry):
            pumped, diag_done = carry
            blk = first + i
            pumped = pump_to(pumped, blk + AHEAD_W)

            def dg(b, _):
                take_diag(b)
                return 0
            diag_to = jnp.minimum(blk + 2, BLOCKS)
            lax.fori_loop(diag_done, diag_to, dg, 0)
            need(blk)
            return pumped, diag_to

        def load(i):
            r = pl.ds(pl.multiple_of((k + i) * RB, RB), RB)
            v = split3(rows_of(first + i, (core, 1 - core)))
            x = split3(jnp.concatenate([x_buf[core, r, :], x_buf[1 - core, r, :]], axis=0))
            t = [p.T for p in v]
            w_buf[...] += dot6(t, x)
            return v, t

        def gather_step(i, carry):
            carry = arrive(i, carry)
            v, t = load(i)
            gs = gram([p[:, :RB] for p in t], [p[:RB] for p in v])
            for q in range(3):
                g_part[q] += gs[q]
            return carry

        carry = lax.fori_loop(0, step, gather_step, (pumped, diag_done))
        pumped, diag_done = arrive(step, carry)

        @pl.when(step > 0)
        def _():
            g_copy(n).start()
        v, t = load(step)
        gs = gram(t, v)
        for q in range(3):
            g_last[q] = gs[q]

        @pl.when(step == 0)
        def _():
            t_copy(xcol, 0, x_dev).wait_recv()
            t_copy(xcol, 2, p_dev).start()
            t_copy(pcol, 1, p_dev).wait_recv()
            t_copy(lax.rem(pcol + 2, 4), 2, p_dev).wait_recv()

        @pl.when(step > 0)
        def _():
            g_copy(n).wait_recv()
            for q in range(3):
                g_last[q] += g_part[q] + g_in[lax.rem(n, 2), q]
        lanes = [[lanes_of(g_last[q], par) for par in range(2)] for q in range(3)]
        ts = [merge(factors(k, par), *[rows_par(lanes[q][par], par) for q in range(3)]) for par in range(2)]
        g01 = jnp.concatenate([
            jnp.concatenate([rows_par(lanes[0][1], 0), rows_par(lanes[1][1], 0)], axis=1),
            jnp.concatenate([rows_par(lanes[1][0], 1).T, rows_par(lanes[2][1], 0)], axis=1)], axis=0)
        w0, w1 = [jnp.concatenate([w_buf[e * 128 + par * PW:e * 128 + (par + 1) * PW, :] for e in range(4)], axis=0)
                  for par in range(2)]
        y1 = dot_f32(ts[1], w1)
        y0 = dot_f32(ts[0], w0 - dot_f32(g01, y1))
        for e in range(4):
            for par, y in enumerate((y0, y1)):
                for q, part in enumerate(split3(y[e * PW:(e + 1) * PW])):
                    y_buf[q, e * 128 + par * PW:e * 128 + (par + 1) * PW, :] = part

        def update_step(i, pumped):
            blk = first + i
            pumped = pump_to(pumped, first + n - 1 + AHEAD_W + (i + 1) // 2)
            rx = pl.ds(pl.multiple_of((k + i) * RB, RB), RB)
            delta = dot6(split3(rows_of(blk, (0, 1))), [y_buf[q] for q in range(3)])
            x_buf[0, rx, :] = x_buf[0, rx, :] - delta[:RB]
            x_buf[1, rx, :] = x_buf[1, rx, :] - delta[RB:]

            @pl.when(jnp.logical_and(k == 0, i > 0))
            def _():
                give(i - 1).start()
            return pumped

        pumped = lax.fori_loop(0, n, update_step, pumped)
        return pumped, diag_done

    def give(i):
        r = pl.ds(pl.multiple_of(i * RB, RB), RB)
        return pltpu.make_async_remote_copy(
            src_ref=x_buf.at[orow, r, :],
            dst_ref=out_hbm.at[r, pl.ds(pl.multiple_of(row * COLS, COLS), COLS)],
            send_sem=c_send.at[i], recv_sem=c_recv.at[i], device_id=y_dev, device_id_type=MESH)

    lax.fori_loop(0, GROUPS, group, (0, 0))

    def drain(blk, _):
        for c in own(blk):
            c.wait_send()
        for c in fwd(blk):
            c.wait_send()
        diag(blk).wait_send()
        return 0
    lax.fori_loop(0, BLOCKS, drain, 0)
    t_copy(col, 0, x_dev).wait_send()
    t_copy(col, 1, p_dev).wait_send()
    t_copy(xcol, 2, p_dev).wait_send()
    g_copy(GROUPS).wait_send()

    give(GROUPS - 1).start()
    keep = pltpu.make_async_copy(
        x_buf.at[row], out_hbm.at[:, pl.ds(pl.multiple_of(row * COLS, COLS), COLS)], io_sem.at[2])
    keep.start()
    keep.wait()

    def drain_c(i, _):
        give(i).wait()
        return 0
    lax.fori_loop(0, GROUPS, drain_c, 0)


def solution(mesh):
    def local_apply(v_loc, t_loc, z_loc):
        t_pk = t_loc.reshape(GROUPS, 2, PW, PW).transpose(0, 2, 1, 3).reshape(GROUPS * PW, 2 * PW)
        z_pk = z_loc.reshape(2, ROWS, COLS)
        any_spec = pl.BlockSpec(memory_space=pl.ANY)
        return pl.pallas_call(
            kernel,
            out_shape=jax.ShapeDtypeStruct((ROWS, 2 * COLS), F32),
            in_specs=[any_spec] * 3,
            out_specs=any_spec,
            scratch_shapes=[
                pltpu.VMEM((8, BLOCKS * RB, 128), F32),
                pltpu.VMEM((4, GROUPS * PW, 2 * PW), F32),
                pltpu.VMEM((2, ROWS, COLS), F32),
                pltpu.VMEM((GW, COLS), F32),
                pltpu.VMEM((3, HW, HW), F32),
                pltpu.VMEM((2, 3, HW, HW), F32),
                pltpu.VMEM((3, HW, HW), F32),
                pltpu.VMEM((3, GW, COLS), BF16),
                pltpu.SemaphoreType.DMA((GROUPS,)),
                pltpu.SemaphoreType.DMA((3,)),
                pltpu.SemaphoreType.DMA((3,)),
                pltpu.SemaphoreType.DMA((8, BLOCKS)),
                pltpu.SemaphoreType.DMA((8, BLOCKS)),
                pltpu.SemaphoreType.DMA,
                pltpu.SemaphoreType.DMA((2,)),
                pltpu.SemaphoreType.DMA((GROUPS,)),
                pltpu.SemaphoreType.DMA((GROUPS,)),
                pltpu.SemaphoreType.DMA((3,)),
            ],
            compiler_params=pltpu.CompilerParams(
                collective_id=0, has_side_effects=True, vmem_limit_bytes=VMEM_LIMIT),
            name='panels',
        )(v_loc, t_pk, z_pk)

    return jax.shard_map(local_apply, mesh=mesh,
                         in_specs=(P('row', 'col'), P('col', None, None), P(None, ('col', 'row'))),
                         out_specs=P('row', 'col'), check_vma=False)
```

```python
import jax
import jax.numpy as jnp
from jax import lax
from jax.experimental import pallas as pl
from jax.experimental.pallas import tpu as pltpu
from jax.sharding import PartitionSpec as P

F32 = jnp.float32
BF16 = jnp.bfloat16
MESH = pl.DeviceIdType.MESH
PW = 64
RB = 256
GROUPS = 8
BLOCKS = GROUPS * (GROUPS + 1) // 2
PACK = 64
STARTS = [n * (n - 1) // 2 for n in range(1, GROUPS + 1)]
Y_ROWS = 128
Y_PACKED = 96
X_ONLY = 28
LAST_GIVES = 2
SPAN = 2 * RB
AHEAD_W = 5
X_LEAD = 4
Y_LEAD = 6
COLS = 256
ROWS = 2048
GW = GROUPS * PW
HW = GW // 2
VMEM_LIMIT = 66 * 10**6


def split3(x):
    a = x.astype(BF16)
    r = x - a.astype(F32)
    b = r.astype(BF16)
    c = (r - b.astype(F32)).astype(BF16)
    return a, b, c


def dot6(lhs, rhs):
    a1, a2, a3 = lhs
    b1, b2, b3 = rhs

    def mm(p, q):
        return jnp.dot(p, q, preferred_element_type=F32)

    return ((mm(a3, b1) + mm(a1, b3)) + mm(a2, b2)) + (mm(a2, b1) + mm(a1, b2)) + mm(a1, b1)


def dot_f32(a, b):
    return dot6(split3(a), split3(b))


def kernel(v_hbm, t_hbm, z_hbm, out_hbm, v_buf, t_own, t_buf, x_buf, w_buf, g_part, g_in, g_last, y_buf,
           xb_buf, y_out, y_in, yb_buf, loc_sem, t_send, t_recv, send, recv, g_send, g_recv, c_send, c_recv,
           y_send, y_recv, o_sem, io_sem):
    row = lax.axis_index('row')
    col = lax.axis_index('col')
    orow = 1 - row
    xcol = lax.rem(col + 2, 4)
    core = lax.rem(col, 2)
    pcol = col + 1 - 2 * core
    x_dev, y_dev, p_dev = (row, xcol), (orow, col), (row, pcol)
    me = row * 4 + col
    xs = row * 4 + xcol
    ys = orow * 4 + col
    ds = orow * 4 + xcol

    def vmem(slot, blk, off=0, size=RB):
        return v_buf.at[slot, pl.ds(pl.multiple_of(blk * RB + off, 8), size), :]

    def rcopy(slot, blk, kind, dev, off=0, size=RB):
        return pltpu.make_async_remote_copy(
            src_ref=vmem(slot, blk, off, size), dst_ref=vmem(slot, blk, off, size),
            send_sem=send.at[kind, blk], recv_sem=recv.at[kind, blk], device_id=dev, device_id_type=MESH)

    OX, OY, OP, FX, FY, PX, PY, PD = range(8)

    def folded(blk):
        found = blk == STARTS[0]
        for b in STARTS[1:]:
            found = jnp.logical_or(found, blk == b)
        return found

    def whole(slot, blk, kind, dev, act):
        if isinstance(blk, int):
            off = PACK if blk in STARTS else 0
            act(rcopy(slot, blk, kind, dev, off, RB - off))
            return
        fold = folded(blk)

        @pl.when(fold)
        def _():
            act(rcopy(slot, blk, kind, dev, PACK, RB - PACK))

        @pl.when(jnp.logical_not(fold))
        def _():
            act(rcopy(slot, blk, kind, dev))

    def own_x(blk, act):
        whole(me, blk, OX, x_dev, act)
        whole(me, blk, OP, p_dev, act)

    def own_y(blk, act):
        whole(me, blk, OY, y_dev, act)

    def mates(blk, act):
        whole(xs, blk, PX, p_dev, act)
        whole(ys, blk, PY, p_dev, act)

    def cross(blk, ys_slot, xs_slot, act):
        fold = folded(blk)

        @pl.when(jnp.logical_and(blk < X_ONLY, fold))
        def _():
            act(rcopy(xs_slot, blk, FY, y_dev, PACK, Y_PACKED))
            act(rcopy(ys_slot, blk, FX, x_dev, PACK + Y_PACKED, RB - PACK - Y_PACKED))

        @pl.when(jnp.logical_and(blk < X_ONLY, jnp.logical_not(fold)))
        def _():
            act(rcopy(xs_slot, blk, FY, y_dev, 0, Y_ROWS))
            act(rcopy(ys_slot, blk, FX, x_dev, Y_ROWS, RB - Y_ROWS))

        @pl.when(blk >= X_ONLY)
        def _():
            whole(ys_slot, blk, FX, x_dev, act)

    def diag(blk, act):
        whole(ds, blk, PD, p_dev, act)

    start = lambda c: c.start()
    sent_out = lambda c: c.wait_send()
    landed = lambda c: c.wait_recv()

    def t_copy(slot, kind, dev):
        return pltpu.make_async_remote_copy(
            src_ref=t_buf.at[slot], dst_ref=t_buf.at[slot], send_sem=t_send.at[kind], recv_sem=t_recv.at[kind],
            device_id=dev, device_id_type=MESH)

    def local_v(n):
        k = GROUPS - n
        o = n * (n - 1) // 2
        return pltpu.make_async_copy(
            v_hbm.at[pl.ds(RB * k, RB * n), pl.ds(2 * PW * k, 2 * PW)],
            v_buf.at[me, pl.ds(RB * o, RB * n), :], loc_sem.at[n - 1])

    t_in = pltpu.make_async_copy(t_hbm, t_own, io_sem.at[0])
    z_in = pltpu.make_async_copy(z_hbm, x_buf, io_sem.at[1])
    soon = 4
    t_in.start()
    for n in range(1, soon + 1):
        local_v(n).start()

    barrier = pltpu.get_barrier_semaphore()
    for dev in (x_dev, y_dev, p_dev):
        pl.semaphore_signal(barrier, inc=1, device_id=dev, device_id_type=MESH)
    t_in.wait()
    for k in range(GROUPS):
        t_buf[col, k * PW:(k + 1) * PW, :] = jnp.concatenate(
            [t_own[2 * k * PW:(2 * k + 1) * PW, :], t_own[(2 * k + 1) * PW:(2 * k + 2) * PW, :]], axis=1)
    half_lane = lax.broadcasted_iota(jnp.int32, (PW, 128), 1) < PW

    def fold_own(n):
        r = RB * STARTS[n - 1]
        low = v_buf[me, r:r + PW, :]
        high = v_buf[me, r + PW:r + 2 * PW, :]
        v_buf[me, r + PW:r + 2 * PW, :] = jnp.where(half_lane, low, pltpu.roll(high, PW, 1))

    for n in range(1, soon + 1):
        local_v(n).wait()
        fold_own(n)
    for m in range(soon + 1, GROUPS + 1):
        local_v(m).start()
    z_in.start()
    pl.semaphore_wait(barrier, 3)

    for b in range(max(X_LEAD, Y_LEAD)):
        if b < X_LEAD:
            own_x(b, start)
        if b < Y_LEAD:
            own_y(b, start)
        if b == 1:
            t_copy(col, 0, x_dev).start()
            t_copy(col, 1, p_dev).start()
    for m in range(soon + 1, GROUPS + 1):
        local_v(m).wait()
        fold_own(m)
    z_in.wait()

    def pump(blk, _):
        whole(xs, blk, OX, x_dev, landed)
        whole(ys, blk, OY, y_dev, landed)
        cross(blk, ys, xs, start)
        mates(blk, start)

        @pl.when(blk + X_LEAD < BLOCKS)
        def _():
            own_x(blk + X_LEAD, start)

        @pl.when(blk + Y_LEAD < BLOCKS)
        def _():
            own_y(blk + Y_LEAD, start)
        return 0

    def pump_to(done, target):
        target = jnp.maximum(done, jnp.minimum(target, BLOCKS))
        lax.fori_loop(done, target, pump, 0)
        return target

    def take_diag(blk):
        cross(blk, ds, ds, landed)
        diag(blk, start)

    def need(blk):
        for kind in (OP, PX, PY, PD):
            whole(me, blk, kind, p_dev, landed)

    def unfold(t, fold):
        p = t[PW:2 * PW]
        top = jnp.concatenate(
            [jnp.where(half_lane, p, 0.0), jnp.where(half_lane, pltpu.roll(p, PW, 1), 0.0)], axis=0)
        return jnp.concatenate([jnp.where(fold, top, t[:2 * PW]), t[2 * PW:]], axis=0)

    def rows_of(blk, dds, fold):
        r = pl.ds(pl.multiple_of(blk * RB, RB), RB)
        return jnp.concatenate(
            [jnp.concatenate([unfold(v_buf[dd * 4 + e, r, :], fold) for e in range(4)], axis=1) for dd in dds], axis=0)

    def gram(cols, vals):
        first = [t[:HW] for t in cols]
        last = [t[HW:] for t in cols]
        vf = [v[:, :HW] for v in vals]
        vl = [v[:, HW:] for v in vals]
        return dot6(first, vf), dot6(first, vl), dot6(last, vl)

    lane = lax.broadcasted_iota(jnp.int32, (HW, 128), 1)
    lane_t = lax.broadcasted_iota(jnp.int32, (PW, 128), 1)
    zero_t = jnp.zeros((PW, 128), F32)

    def lanes_of(q, par):
        a, b = q[:, :128], q[:, 128:]
        if par == 0:
            return jnp.where(lane < PW, a, pltpu.roll(b, PW, 1))
        return jnp.where(lane < PW, pltpu.roll(a, PW, 1), b)

    def rows_par(q, par):
        return jnp.concatenate([q[par * PW:(par + 1) * PW], q[128 + par * PW:128 + (par + 1) * PW]], axis=0)

    def factors(k, par):
        tiles = []
        for e in range(4):
            t = t_buf[e, pl.ds(pl.multiple_of(k * PW, PW), PW), :]
            src = t if par == e % 2 else pltpu.roll(t, PW, 1)
            tiles.append(jnp.where(lane_t // PW == e % 2, src, 0.0))
        return tiles

    def diag256(tiles):
        return jnp.concatenate(
            [jnp.concatenate([t, zero_t] if e < 2 else [zero_t, t], axis=1) for e, t in enumerate(tiles)], axis=0)

    def merge(tiles, gaa, gab, gbb):
        whole = diag256(tiles)
        u = jnp.concatenate([jnp.where(lane_t < PW, 0.0, gaa[:PW]), jnp.where(lane_t < PW, 0.0, gbb[:PW])], axis=1)
        c = dot_f32(u, whole)
        rhs = jnp.concatenate([
            jnp.concatenate([c[:, :128], zero_t], axis=1), jnp.zeros((PW, HW), F32),
            jnp.concatenate([zero_t, c[:, 128:]], axis=1), jnp.zeros((PW, HW), F32)], axis=0)
        lhs = jnp.concatenate([tiles[0] + tiles[1], tiles[2] + tiles[3]], axis=1)
        p = dot_f32(lhs, rhs)
        ta = jnp.concatenate([tiles[0] - p[:, :128], tiles[1]], axis=0)
        tb = jnp.concatenate([tiles[2] - p[:, 128:], tiles[3]], axis=0)
        tab = dot_f32(ta, dot_f32(gab, tb))
        return jnp.concatenate([
            jnp.concatenate([ta, -tab], axis=1), jnp.concatenate([jnp.zeros_like(tb), tb], axis=1)], axis=0)

    def g_copy(n):
        return pltpu.make_async_remote_copy(
            src_ref=g_part, dst_ref=g_in.at[lax.rem(n, 2)], send_sem=g_send, recv_sem=g_recv.at[lax.rem(n, 2)],
            device_id=p_dev, device_id_type=MESH)

    def group(step, carry):
        pumped, diag_done = carry
        n = step + 1
        k = GROUPS - n
        first = n * step // 2
        w_buf[...] = jnp.zeros_like(w_buf)

        @pl.when(n > 2)
        def _():
            g_copy(n - 1).wait_send()
        g_part[...] = jnp.zeros_like(g_part)

        def arrive(i, carry):
            pumped, diag_done = carry
            blk = first + i
            pumped = pump_to(pumped, blk + AHEAD_W)

            def dg(b, _):
                take_diag(b)
                return 0
            diag_to = jnp.minimum(blk + 2, BLOCKS)
            lax.fori_loop(diag_done, diag_to, dg, 0)
            need(blk)
            return pumped, diag_to

        def load(i):
            r = pl.ds(pl.multiple_of((k + i) * RB, RB), RB)
            v = split3(rows_of(first + i, (core, 1 - core), i == 0))
            x = split3(jnp.concatenate([x_buf[core, r, :], x_buf[1 - core, r, :]], axis=0))
            t = [p.T for p in v]
            w_buf[...] += dot6(t, x)
            return v, t

        def gather_step(i, carry):
            carry = arrive(i, carry)
            v, t = load(i)
            gs = gram([p[:, :RB] for p in t], [p[:RB] for p in v])
            for q in range(3):
                g_part[q] += gs[q]
            return carry

        carry = lax.fori_loop(0, step, gather_step, (pumped, diag_done))
        pumped, diag_done = arrive(step, carry)

        @pl.when(step > 0)
        def _():
            g_copy(n).start()
        v, t = load(step)
        gs = gram(t, v)
        for q in range(3):
            g_last[q] = gs[q]

        @pl.when(step == 0)
        def _():
            t_copy(xcol, 0, x_dev).wait_recv()
            t_copy(xcol, 2, p_dev).start()
            t_copy(pcol, 1, p_dev).wait_recv()
            t_copy(lax.rem(pcol + 2, 4), 2, p_dev).wait_recv()

        @pl.when(step > 0)
        def _():
            g_copy(n).wait_recv()
            for q in range(3):
                g_last[q] += g_part[q] + g_in[lax.rem(n, 2), q]
        lanes = [[lanes_of(g_last[q], par) for par in range(2)] for q in range(3)]
        ts = [merge(factors(k, par), *[rows_par(lanes[q][par], par) for q in range(3)]) for par in range(2)]
        g01 = jnp.concatenate([
            jnp.concatenate([rows_par(lanes[0][1], 0), rows_par(lanes[1][1], 0)], axis=1),
            jnp.concatenate([rows_par(lanes[1][0], 1).T, rows_par(lanes[2][1], 0)], axis=1)], axis=0)
        w0, w1 = [jnp.concatenate([w_buf[e * 128 + par * PW:e * 128 + (par + 1) * PW, :] for e in range(4)], axis=0)
                  for par in range(2)]
        y1 = dot_f32(ts[1], w1)
        y0 = dot_f32(ts[0], w0 - dot_f32(g01, y1))
        @pl.when(k == 0)
        def _():
            for e in range(4):
                for par, y in enumerate((y0, y1)):
                    y_out[e * 128 + par * PW:e * 128 + (par + 1) * PW, :] = y[e * PW:(e + 1) * PW]
        for e in range(4):
            for par, y in enumerate((y0, y1)):
                for q, part in enumerate(split3(y[e * PW:(e + 1) * PW])):
                    y_buf[q, e * 128 + par * PW:e * 128 + (par + 1) * PW, :] = part

        def update_step(i, pumped):
            blk = first + i
            pumped = pump_to(pumped, first + n - 1 + AHEAD_W + (i + 1) // 2)
            rx = pl.ds(pl.multiple_of((k + i) * RB, RB), RB)
            delta = dot6(split3(rows_of(blk, (0, 1), i == 0)), [y_buf[q] for q in range(3)])
            x_buf[0, rx, :] = x_buf[0, rx, :] - delta[:RB]
            x_buf[1, rx, :] = x_buf[1, rx, :] - delta[RB:]

            @pl.when(jnp.logical_and(k == 1, i < GROUPS - LAST_GIVES))
            def _():
                give(i).start()
            return pumped

        pumped = lax.fori_loop(0, jnp.where(k == 0, 0, n), update_step, pumped)
        return pumped, diag_done

    def give(i):
        r = pl.ds(pl.multiple_of(i * RB, RB), RB)
        return pltpu.make_async_remote_copy(
            src_ref=x_buf.at[orow, r, :], dst_ref=xb_buf.at[r, :], send_sem=c_send.at[i], recv_sem=c_recv.at[i],
            device_id=y_dev, device_id_type=MESH)

    y_copy = pltpu.make_async_remote_copy(
        src_ref=y_out, dst_ref=y_in, send_sem=y_send, recv_sem=y_recv, device_id=y_dev, device_id_type=MESH)

    lax.fori_loop(0, GROUPS, group, (0, 0))

    first_last = BLOCKS - GROUPS

    def span_of(i):
        return pl.ds(pl.multiple_of(i * SPAN, SPAN), SPAN)

    def v_span(i):
        r = pl.ds(pl.multiple_of(first_last * RB + i * SPAN, SPAN), SPAN)
        return split3(jnp.concatenate([unfold(v_buf[row * 4 + e, r, :], i == 0) for e in range(4)], axis=1))

    def put(i, side):
        at = row if side == 0 else orow
        src = x_buf.at[row, span_of(i), :] if side == 0 else xb_buf.at[span_of(i), :]
        return pltpu.make_async_copy(
            src, out_hbm.at[span_of(i), pl.ds(pl.multiple_of(at * COLS, COLS), COLS)], o_sem.at[side, i])

    spans = ROWS // SPAN

    def mine(i, _):
        x_buf[row, span_of(i), :] = x_buf[row, span_of(i), :] - dot6(v_span(i), [y_buf[q] for q in range(3)])

        @pl.when(i == 0)
        def _():
            y_copy.start()
            for g in range(GROUPS - LAST_GIVES, GROUPS):
                give(g).start()

        @pl.when(i > 0)
        def _():
            put(i - 1, 0).start()
        return 0
    lax.fori_loop(0, spans, mine, 0)

    y_copy.wait_recv()
    for q, part in enumerate(split3(y_in[...])):
        yb_buf[q] = part
    put(spans - 1, 0).start()

    def theirs(i, _):
        for h in range(SPAN // RB):
            give(i * (SPAN // RB) + h).wait_recv()
        xb_buf[span_of(i), :] = xb_buf[span_of(i), :] - dot6(v_span(i), [yb_buf[q] for q in range(3)])

        @pl.when(i > 0)
        def _():
            put(i - 1, 1).start()
        return 0
    lax.fori_loop(0, spans, theirs, 0)

    def drain(blk, _):
        own_x(blk, sent_out)
        own_y(blk, sent_out)
        cross(blk, ys, xs, sent_out)
        mates(blk, sent_out)
        diag(blk, sent_out)
        return 0
    lax.fori_loop(0, BLOCKS, drain, 0)
    t_copy(col, 0, x_dev).wait_send()
    t_copy(col, 1, p_dev).wait_send()
    t_copy(xcol, 2, p_dev).wait_send()
    g_copy(GROUPS).wait_send()


    put(spans - 1, 1).start()
    y_copy.wait_send()

    def drain_c(i, _):
        give(i).wait_send()
        return 0
    lax.fori_loop(0, GROUPS, drain_c, 0)
    for i in range(spans):
        put(i, 0).wait()
        put(i, 1).wait()


def solution(mesh):
    def local_apply(v_loc, t_loc, z_loc):
        t_pk = t_loc.reshape(2 * GROUPS * PW, PW)
        z_pk = z_loc.reshape(2, ROWS, COLS)
        any_spec = pl.BlockSpec(memory_space=pl.ANY)
        return pl.pallas_call(
            kernel,
            out_shape=jax.ShapeDtypeStruct((ROWS, 2 * COLS), F32),
            in_specs=[any_spec] * 3,
            out_specs=any_spec,
            scratch_shapes=[
                pltpu.VMEM((8, BLOCKS * RB, 128), F32),
                pltpu.VMEM((2 * GROUPS * PW, PW), F32),
                pltpu.VMEM((4, GROUPS * PW, 2 * PW), F32),
                pltpu.VMEM((2, ROWS, COLS), F32),
                pltpu.VMEM((GW, COLS), F32),
                pltpu.VMEM((3, HW, HW), F32),
                pltpu.VMEM((2, 3, HW, HW), F32),
                pltpu.VMEM((3, HW, HW), F32),
                pltpu.VMEM((3, GW, COLS), BF16),
                pltpu.VMEM((ROWS, COLS), F32),
                pltpu.VMEM((GW, COLS), F32),
                pltpu.VMEM((GW, COLS), F32),
                pltpu.VMEM((3, GW, COLS), BF16),
                pltpu.SemaphoreType.DMA((GROUPS,)),
                pltpu.SemaphoreType.DMA((3,)),
                pltpu.SemaphoreType.DMA((3,)),
                pltpu.SemaphoreType.DMA((8, BLOCKS)),
                pltpu.SemaphoreType.DMA((8, BLOCKS)),
                pltpu.SemaphoreType.DMA,
                pltpu.SemaphoreType.DMA((2,)),
                pltpu.SemaphoreType.DMA((GROUPS,)),
                pltpu.SemaphoreType.DMA((GROUPS,)),
                pltpu.SemaphoreType.DMA,
                pltpu.SemaphoreType.DMA,
                pltpu.SemaphoreType.DMA((2, ROWS // SPAN)),
                pltpu.SemaphoreType.DMA((2,)),
            ],
            compiler_params=pltpu.CompilerParams(
                collective_id=0, has_side_effects=True, vmem_limit_bytes=VMEM_LIMIT),
            name='panels',
        )(v_loc, t_pk, z_pk)

    return jax.shard_map(local_apply, mesh=mesh,
                         in_specs=(P('row', 'col'), P('col', None, None), P(None, ('col', 'row'))),
                         out_specs=P('row', 'col'), check_vma=False)
```

```python
import jax
import jax.numpy as jnp
from jax import lax
from jax.experimental import pallas as pl
from jax.experimental.pallas import tpu as pltpu
from jax.sharding import PartitionSpec as P

F32 = jnp.float32
BF16 = jnp.bfloat16
MESH = pl.DeviceIdType.MESH
PW = 64
RB = 256
GROUPS = 8
BLOCKS = GROUPS * (GROUPS + 1) // 2
PACK = 64
STARTS = [n * (n - 1) // 2 for n in range(1, GROUPS + 1)]
Y_ROWS = 128
Y_PACKED = 96
X_ONLY = 30
LAST_GIVES = 2
SPAN = 2 * RB
AHEAD_W = 5
X_LEAD = 4
Y_LEAD = 6
COLS = 256
ROWS = 2048
GW = GROUPS * PW
HW = GW // 2
VMEM_LIMIT = 60 * 10**6


def split3(x):
    a = x.astype(BF16)
    r = x - a.astype(F32)
    b = r.astype(BF16)
    c = (r - b.astype(F32)).astype(BF16)
    return a, b, c


def dot6(lhs, rhs):
    a1, a2, a3 = lhs
    b1, b2, b3 = rhs

    def mm(p, q):
        return jnp.dot(p, q, preferred_element_type=F32)

    return ((mm(a3, b1) + mm(a1, b3)) + mm(a2, b2)) + (mm(a2, b1) + mm(a1, b2)) + mm(a1, b1)


def dot_f32(a, b):
    return dot6(split3(a), split3(b))


def kernel(v_hbm, t_hbm, z_hbm, out_ref, v_buf, t_own, t_buf, x_buf, w_buf, g_part, g_in, g_last, y_buf,
           xb_buf, y_out, y_in, yb_buf, loc_sem, t_send, t_recv, send, recv, g_send, g_recv, c_send, c_recv,
           y_send, y_recv, io_sem):
    row = lax.axis_index('row')
    col = lax.axis_index('col')
    orow = 1 - row
    xcol = lax.rem(col + 2, 4)
    core = lax.rem(col, 2)
    pcol = col + 1 - 2 * core
    x_dev, y_dev, p_dev = (row, xcol), (orow, col), (row, pcol)
    me = row * 4 + col
    xs = row * 4 + xcol
    ys = orow * 4 + col
    ds = orow * 4 + xcol

    def vmem(slot, blk, off=0, size=RB):
        return v_buf.at[slot, pl.ds(pl.multiple_of(blk * RB + off, 8), size), :]

    def rcopy(slot, blk, kind, dev, off=0, size=RB):
        return pltpu.make_async_remote_copy(
            src_ref=vmem(slot, blk, off, size), dst_ref=vmem(slot, blk, off, size),
            send_sem=send.at[kind, blk], recv_sem=recv.at[kind, blk], device_id=dev, device_id_type=MESH)

    OX, OY, OP, FX, FY, PX, PY, PD = range(8)

    def folded(blk):
        found = blk == STARTS[0]
        for b in STARTS[1:]:
            found = jnp.logical_or(found, blk == b)
        return found

    def whole(slot, blk, kind, dev, act):
        if isinstance(blk, int):
            off = PACK if blk in STARTS else 0
            act(rcopy(slot, blk, kind, dev, off, RB - off))
            return
        fold = folded(blk)

        @pl.when(fold)
        def _():
            act(rcopy(slot, blk, kind, dev, PACK, RB - PACK))

        @pl.when(jnp.logical_not(fold))
        def _():
            act(rcopy(slot, blk, kind, dev))

    def own_x(blk, act):
        whole(me, blk, OX, x_dev, act)
        whole(me, blk, OP, p_dev, act)

    def own_y(blk, act):
        whole(me, blk, OY, y_dev, act)

    def mates(blk, act):
        whole(xs, blk, PX, p_dev, act)
        whole(ys, blk, PY, p_dev, act)

    def cross(blk, ys_slot, xs_slot, act):
        fold = folded(blk)

        @pl.when(jnp.logical_and(blk < X_ONLY, fold))
        def _():
            act(rcopy(xs_slot, blk, FY, y_dev, PACK, Y_PACKED))
            act(rcopy(ys_slot, blk, FX, x_dev, PACK + Y_PACKED, RB - PACK - Y_PACKED))

        @pl.when(jnp.logical_and(blk < X_ONLY, jnp.logical_not(fold)))
        def _():
            act(rcopy(xs_slot, blk, FY, y_dev, 0, Y_ROWS))
            act(rcopy(ys_slot, blk, FX, x_dev, Y_ROWS, RB - Y_ROWS))

        @pl.when(blk >= X_ONLY)
        def _():
            whole(ys_slot, blk, FX, x_dev, act)

    def diag(blk, act):
        whole(ds, blk, PD, p_dev, act)

    start = lambda c: c.start()
    sent_out = lambda c: c.wait_send()
    landed = lambda c: c.wait_recv()

    def t_copy(slot, kind, dev):
        return pltpu.make_async_remote_copy(
            src_ref=t_buf.at[slot], dst_ref=t_buf.at[slot], send_sem=t_send.at[kind], recv_sem=t_recv.at[kind],
            device_id=dev, device_id_type=MESH)

    def local_v(n):
        k = GROUPS - n
        o = n * (n - 1) // 2
        return pltpu.make_async_copy(
            v_hbm.at[pl.ds(RB * k, RB * n), pl.ds(2 * PW * k, 2 * PW)],
            v_buf.at[me, pl.ds(RB * o, RB * n), :], loc_sem.at[n - 1])

    t_in = pltpu.make_async_copy(t_hbm, t_own, io_sem.at[0])
    z_in = pltpu.make_async_copy(z_hbm, x_buf, io_sem.at[1])
    soon = 4
    t_in.start()
    for n in range(1, soon + 1):
        local_v(n).start()

    barrier = pltpu.get_barrier_semaphore()
    for dev in (x_dev, y_dev, p_dev):
        pl.semaphore_signal(barrier, inc=1, device_id=dev, device_id_type=MESH)
    t_in.wait()
    for k in range(GROUPS):
        t_buf[col, k * PW:(k + 1) * PW, :] = jnp.concatenate(
            [t_own[2 * k * PW:(2 * k + 1) * PW, :], t_own[(2 * k + 1) * PW:(2 * k + 2) * PW, :]], axis=1)
    half_lane = lax.broadcasted_iota(jnp.int32, (PW, 128), 1) < PW

    def fold_own(n):
        r = RB * STARTS[n - 1]
        low = v_buf[me, r:r + PW, :]
        high = v_buf[me, r + PW:r + 2 * PW, :]
        v_buf[me, r + PW:r + 2 * PW, :] = jnp.where(half_lane, low, pltpu.roll(high, PW, 1))

    for n in range(1, soon + 1):
        local_v(n).wait()
        fold_own(n)
    for m in range(soon + 1, GROUPS + 1):
        local_v(m).start()
    z_in.start()
    pl.semaphore_wait(barrier, 3)

    for b in range(max(X_LEAD, Y_LEAD)):
        if b < X_LEAD:
            own_x(b, start)
        if b < Y_LEAD:
            own_y(b, start)
        if b == 1:
            t_copy(col, 0, x_dev).start()
            t_copy(col, 1, p_dev).start()
    for m in range(soon + 1, GROUPS + 1):
        local_v(m).wait()
        fold_own(m)
    z_in.wait()

    def pump(blk, _):
        whole(xs, blk, OX, x_dev, landed)
        whole(ys, blk, OY, y_dev, landed)
        cross(blk, ys, xs, start)
        mates(blk, start)

        @pl.when(blk + X_LEAD < BLOCKS)
        def _():
            own_x(blk + X_LEAD, start)

        @pl.when(blk + Y_LEAD < BLOCKS)
        def _():
            own_y(blk + Y_LEAD, start)
        return 0

    def pump_to(done, target):
        target = jnp.maximum(done, jnp.minimum(target, BLOCKS))
        lax.fori_loop(done, target, pump, 0)
        return target

    def take_diag(blk):
        cross(blk, ds, ds, landed)
        diag(blk, start)

    def need(blk):
        for kind in (OP, PX, PY, PD):
            whole(me, blk, kind, p_dev, landed)

    def unfold(t, fold):
        p = t[PW:2 * PW]
        top = jnp.concatenate(
            [jnp.where(half_lane, p, 0.0), jnp.where(half_lane, pltpu.roll(p, PW, 1), 0.0)], axis=0)
        return jnp.concatenate([jnp.where(fold, top, t[:2 * PW]), t[2 * PW:]], axis=0)

    def rows_of(blk, dds, fold):
        r = pl.ds(pl.multiple_of(blk * RB, RB), RB)
        return jnp.concatenate(
            [jnp.concatenate([unfold(v_buf[dd * 4 + e, r, :], fold) for e in range(4)], axis=1) for dd in dds], axis=0)

    def gram(cols, vals):
        first = [t[:HW] for t in cols]
        last = [t[HW:] for t in cols]
        vf = [v[:, :HW] for v in vals]
        vl = [v[:, HW:] for v in vals]
        return dot6(first, vf), dot6(first, vl), dot6(last, vl)

    lane = lax.broadcasted_iota(jnp.int32, (HW, 128), 1)
    lane_t = lax.broadcasted_iota(jnp.int32, (PW, 128), 1)
    zero_t = jnp.zeros((PW, 128), F32)

    def lanes_of(q, par):
        a, b = q[:, :128], q[:, 128:]
        if par == 0:
            return jnp.where(lane < PW, a, pltpu.roll(b, PW, 1))
        return jnp.where(lane < PW, pltpu.roll(a, PW, 1), b)

    def rows_par(q, par):
        return jnp.concatenate([q[par * PW:(par + 1) * PW], q[128 + par * PW:128 + (par + 1) * PW]], axis=0)

    def factors(k, par):
        tiles = []
        for e in range(4):
            t = t_buf[e, pl.ds(pl.multiple_of(k * PW, PW), PW), :]
            src = t if par == e % 2 else pltpu.roll(t, PW, 1)
            tiles.append(jnp.where(lane_t // PW == e % 2, src, 0.0))
        return tiles

    def diag256(tiles):
        return jnp.concatenate(
            [jnp.concatenate([t, zero_t] if e < 2 else [zero_t, t], axis=1) for e, t in enumerate(tiles)], axis=0)

    def merge(tiles, gaa, gab, gbb):
        whole = diag256(tiles)
        u = jnp.concatenate([jnp.where(lane_t < PW, 0.0, gaa[:PW]), jnp.where(lane_t < PW, 0.0, gbb[:PW])], axis=1)
        c = dot_f32(u, whole)
        rhs = jnp.concatenate([
            jnp.concatenate([c[:, :128], zero_t], axis=1), jnp.zeros((PW, HW), F32),
            jnp.concatenate([zero_t, c[:, 128:]], axis=1), jnp.zeros((PW, HW), F32)], axis=0)
        lhs = jnp.concatenate([tiles[0] + tiles[1], tiles[2] + tiles[3]], axis=1)
        p = dot_f32(lhs, rhs)
        ta = jnp.concatenate([tiles[0] - p[:, :128], tiles[1]], axis=0)
        tb = jnp.concatenate([tiles[2] - p[:, 128:], tiles[3]], axis=0)
        tab = dot_f32(ta, dot_f32(gab, tb))
        return jnp.concatenate([
            jnp.concatenate([ta, -tab], axis=1), jnp.concatenate([jnp.zeros_like(tb), tb], axis=1)], axis=0)

    def g_copy(n):
        return pltpu.make_async_remote_copy(
            src_ref=g_part, dst_ref=g_in.at[lax.rem(n, 2)], send_sem=g_send, recv_sem=g_recv.at[lax.rem(n, 2)],
            device_id=p_dev, device_id_type=MESH)

    def group(step, carry):
        pumped, diag_done = carry
        n = step + 1
        k = GROUPS - n
        first = n * step // 2
        w_buf[...] = jnp.zeros_like(w_buf)

        @pl.when(n > 2)
        def _():
            g_copy(n - 1).wait_send()
        g_part[...] = jnp.zeros_like(g_part)

        def arrive(i, carry, pumping=True):
            pumped, diag_done = carry
            blk = first + i
            if pumping:
                pumped = pump_to(pumped, blk + AHEAD_W)

            def dg(b, _):
                take_diag(b)
                return 0
            diag_to = jnp.minimum(blk + 2, BLOCKS)
            lax.fori_loop(diag_done, diag_to, dg, 0)
            need(blk)
            return pumped, diag_to

        def load(i):
            r = pl.ds(pl.multiple_of((k + i) * RB, RB), RB)
            v = split3(rows_of(first + i, (core, 1 - core), i == 0))
            x = split3(jnp.concatenate([x_buf[core, r, :], x_buf[1 - core, r, :]], axis=0))
            t = [p.T for p in v]
            w_buf[...] += dot6(t, x)
            return v, t

        def gather_step(i, carry):
            carry = arrive(i, carry, False)
            v, t = load(i)
            gs = gram([p[:, :RB] for p in t], [p[:RB] for p in v])
            for q in range(3):
                g_part[q] += gs[q]
            pumped, diag_done = carry
            return pump_to(pumped, first + i + 1 + AHEAD_W), diag_done

        carry = lax.fori_loop(0, step, gather_step, (pumped, diag_done))
        pumped, diag_done = arrive(step, carry)

        @pl.when(step > 0)
        def _():
            g_copy(n).start()
        v, t = load(step)
        gs = gram(t, v)
        for q in range(3):
            g_last[q] = gs[q]

        @pl.when(step == 0)
        def _():
            t_copy(xcol, 0, x_dev).wait_recv()
            t_copy(xcol, 2, p_dev).start()
            t_copy(pcol, 1, p_dev).wait_recv()
            t_copy(lax.rem(pcol + 2, 4), 2, p_dev).wait_recv()

        @pl.when(step > 0)
        def _():
            g_copy(n).wait_recv()
            for q in range(3):
                g_last[q] += g_part[q] + g_in[lax.rem(n, 2), q]
        lanes = [[lanes_of(g_last[q], par) for par in range(2)] for q in range(3)]
        ts = [merge(factors(k, par), *[rows_par(lanes[q][par], par) for q in range(3)]) for par in range(2)]
        g01 = jnp.concatenate([
            jnp.concatenate([rows_par(lanes[0][1], 0), rows_par(lanes[1][1], 0)], axis=1),
            jnp.concatenate([rows_par(lanes[1][0], 1).T, rows_par(lanes[2][1], 0)], axis=1)], axis=0)
        w0, w1 = [jnp.concatenate([w_buf[e * 128 + par * PW:e * 128 + (par + 1) * PW, :] for e in range(4)], axis=0)
                  for par in range(2)]
        y1 = dot_f32(ts[1], w1)
        y0 = dot_f32(ts[0], w0 - dot_f32(g01, y1))
        @pl.when(k == 0)
        def _():
            for e in range(4):
                for par, y in enumerate((y0, y1)):
                    y_out[e * 128 + par * PW:e * 128 + (par + 1) * PW, :] = y[e * PW:(e + 1) * PW]
        for e in range(4):
            for par, y in enumerate((y0, y1)):
                for q, part in enumerate(split3(y[e * PW:(e + 1) * PW])):
                    y_buf[q, e * 128 + par * PW:e * 128 + (par + 1) * PW, :] = part

        def update_step(i, pumped):
            blk = first + i
            pumped = pump_to(pumped, first + n - 1 + AHEAD_W + (i + 1) // 2)
            rx = pl.ds(pl.multiple_of((k + i) * RB, RB), RB)
            delta = dot6(split3(rows_of(blk, (0, 1), i == 0)), [y_buf[q] for q in range(3)])
            x_buf[0, rx, :] = x_buf[0, rx, :] - delta[:RB]
            x_buf[1, rx, :] = x_buf[1, rx, :] - delta[RB:]

            @pl.when(jnp.logical_and(k == 1, i < GROUPS - LAST_GIVES))
            def _():
                give(i).start()
            return pumped

        pumped = lax.fori_loop(0, jnp.where(k == 0, 0, n), update_step, pumped)
        return pumped, diag_done

    def give(i):
        r = pl.ds(pl.multiple_of(i * RB, RB), RB)
        return pltpu.make_async_remote_copy(
            src_ref=x_buf.at[orow, r, :], dst_ref=xb_buf.at[r, :], send_sem=c_send.at[i], recv_sem=c_recv.at[i],
            device_id=y_dev, device_id_type=MESH)

    y_copy = pltpu.make_async_remote_copy(
        src_ref=y_out, dst_ref=y_in, send_sem=y_send, recv_sem=y_recv, device_id=y_dev, device_id_type=MESH)

    lax.fori_loop(0, GROUPS, group, (0, 0))

    first_last = BLOCKS - GROUPS

    def span_of(i):
        return pl.ds(pl.multiple_of(i * SPAN, SPAN), SPAN)

    def v_span(i):
        r = pl.ds(pl.multiple_of(first_last * RB + i * SPAN, SPAN), SPAN)
        return split3(jnp.concatenate([unfold(v_buf[row * 4 + e, r, :], i == 0) for e in range(4)], axis=1))

    def half_of(i, at):
        return out_ref.at[span_of(i), pl.ds(pl.multiple_of(at * COLS, COLS), COLS)]

    spans = ROWS // SPAN

    def mine(i, _):
        half_of(i, row)[...] = x_buf[row, span_of(i), :] - dot6(v_span(i), [y_buf[q] for q in range(3)])

        @pl.when(i == 0)
        def _():
            y_copy.start()
            for g in range(GROUPS - LAST_GIVES, GROUPS):
                give(g).start()
        return 0
    lax.fori_loop(0, spans, mine, 0)

    y_copy.wait_recv()
    for q, part in enumerate(split3(y_in[...])):
        yb_buf[q] = part

    def theirs(i, _):
        for h in range(SPAN // RB):
            give(i * (SPAN // RB) + h).wait_recv()
        half_of(i, orow)[...] = xb_buf[span_of(i), :] - dot6(v_span(i), [yb_buf[q] for q in range(3)])
        return 0
    lax.fori_loop(0, spans, theirs, 0)

    def drain(blk, _):
        own_x(blk, sent_out)
        own_y(blk, sent_out)
        cross(blk, ys, xs, sent_out)
        mates(blk, sent_out)
        diag(blk, sent_out)
        return 0
    lax.fori_loop(0, BLOCKS, drain, 0)
    t_copy(col, 0, x_dev).wait_send()
    t_copy(col, 1, p_dev).wait_send()
    t_copy(xcol, 2, p_dev).wait_send()
    g_copy(GROUPS).wait_send()


    y_copy.wait_send()

    def drain_c(i, _):
        give(i).wait_send()
        return 0
    lax.fori_loop(0, GROUPS, drain_c, 0)


def solution(mesh):
    def local_apply(v_loc, t_loc, z_loc):
        t_pk = t_loc.reshape(2 * GROUPS * PW, PW)
        z_pk = z_loc.reshape(2, ROWS, COLS)
        any_spec = pl.BlockSpec(memory_space=pl.ANY)
        return pl.pallas_call(
            kernel,
            out_shape=pltpu.VMEM((ROWS, 2 * COLS), F32),
            in_specs=[any_spec] * 3,
            out_specs=pl.BlockSpec(memory_space=pltpu.VMEM),
            scratch_shapes=[
                pltpu.VMEM((8, BLOCKS * RB, 128), F32),
                pltpu.VMEM((2 * GROUPS * PW, PW), F32),
                pltpu.VMEM((4, GROUPS * PW, 2 * PW), F32),
                pltpu.VMEM((2, ROWS, COLS), F32),
                pltpu.VMEM((GW, COLS), F32),
                pltpu.VMEM((3, HW, HW), F32),
                pltpu.VMEM((2, 3, HW, HW), F32),
                pltpu.VMEM((3, HW, HW), F32),
                pltpu.VMEM((3, GW, COLS), BF16),
                pltpu.VMEM((ROWS, COLS), F32),
                pltpu.VMEM((GW, COLS), F32),
                pltpu.VMEM((GW, COLS), F32),
                pltpu.VMEM((3, GW, COLS), BF16),
                pltpu.SemaphoreType.DMA((GROUPS,)),
                pltpu.SemaphoreType.DMA((3,)),
                pltpu.SemaphoreType.DMA((3,)),
                pltpu.SemaphoreType.DMA((8, BLOCKS)),
                pltpu.SemaphoreType.DMA((8, BLOCKS)),
                pltpu.SemaphoreType.DMA,
                pltpu.SemaphoreType.DMA((2,)),
                pltpu.SemaphoreType.DMA((GROUPS,)),
                pltpu.SemaphoreType.DMA((GROUPS,)),
                pltpu.SemaphoreType.DMA,
                pltpu.SemaphoreType.DMA,
                pltpu.SemaphoreType.DMA((2,)),
            ],
            compiler_params=pltpu.CompilerParams(
                collective_id=0, has_side_effects=True, vmem_limit_bytes=VMEM_LIMIT),
            name='panels',
        )(v_loc, t_pk, z_pk)

    return jax.shard_map(local_apply, mesh=mesh,
                         in_specs=(P('row', 'col'), P('col', None, None), P(None, ('col', 'row'))),
                         out_specs=P('row', 'col'), check_vma=False)
```

```python
import jax
import jax.numpy as jnp
from jax import lax
from jax.experimental import pallas as pl
from jax.experimental.pallas import tpu as pltpu
from jax.sharding import PartitionSpec as P

F32 = jnp.float32
BF16 = jnp.bfloat16
MESH = pl.DeviceIdType.MESH
PW = 64
RB = 256
GROUPS = 8
BLOCKS = GROUPS * (GROUPS + 1) // 2
PACK = 64
STARTS = [n * (n - 1) // 2 for n in range(1, GROUPS + 1)]
Y_ROWS = 128
Y_PACKED = 96
X_ONLY = 30
LAST_GIVES = 2
SPAN = RB
AHEAD_W = 5
X_LEAD = 4
Y_LEAD = 6
COLS = 256
ROWS = 2048
GW = GROUPS * PW
HW = GW // 2
VMEM_LIMIT = 60 * 10**6


def split3(x):
    a = x.astype(BF16)
    r = x - a.astype(F32)
    b = r.astype(BF16)
    c = (r - b.astype(F32)).astype(BF16)
    return a, b, c


def dot6(lhs, rhs):
    a1, a2, a3 = lhs
    b1, b2, b3 = rhs

    def mm(p, q):
        return jnp.dot(p, q, preferred_element_type=F32)

    return ((mm(a3, b1) + mm(a1, b3)) + mm(a2, b2)) + (mm(a2, b1) + mm(a1, b2)) + mm(a1, b1)


def dot_f32(a, b):
    return dot6(split3(a), split3(b))


def kernel(v_hbm, t_hbm, z_hbm, out_ref, v_buf, t_own, t_buf, x_buf, w_buf, g_part, g_in, g_last, y_buf,
           xb_buf, y_out, y_in, yb_buf, loc_sem, t_send, t_recv, send, recv, g_send, g_recv, c_send, c_recv,
           y_send, y_recv, io_sem):
    row = lax.axis_index('row')
    col = lax.axis_index('col')
    orow = 1 - row
    xcol = lax.rem(col + 2, 4)
    core = lax.rem(col, 2)
    pcol = col + 1 - 2 * core
    x_dev, y_dev, p_dev = (row, xcol), (orow, col), (row, pcol)
    me = row * 4 + col
    xs = row * 4 + xcol
    ys = orow * 4 + col
    ds = orow * 4 + xcol

    def vmem(slot, blk, off=0, size=RB):
        return v_buf.at[slot, pl.ds(pl.multiple_of(blk * RB + off, 8), size), :]

    def rcopy(slot, blk, kind, dev, off=0, size=RB):
        return pltpu.make_async_remote_copy(
            src_ref=vmem(slot, blk, off, size), dst_ref=vmem(slot, blk, off, size),
            send_sem=send.at[kind, blk], recv_sem=recv.at[kind, blk], device_id=dev, device_id_type=MESH)

    OX, OY, OP, FX, FY, PX, PY, PD = range(8)

    def folded(blk):
        found = blk == STARTS[0]
        for b in STARTS[1:]:
            found = jnp.logical_or(found, blk == b)
        return found

    def whole(slot, blk, kind, dev, act):
        if isinstance(blk, int):
            off = PACK if blk in STARTS else 0
            act(rcopy(slot, blk, kind, dev, off, RB - off))
            return
        fold = folded(blk)

        @pl.when(fold)
        def _():
            act(rcopy(slot, blk, kind, dev, PACK, RB - PACK))

        @pl.when(jnp.logical_not(fold))
        def _():
            act(rcopy(slot, blk, kind, dev))

    def own_x(blk, act):
        whole(me, blk, OX, x_dev, act)
        whole(me, blk, OP, p_dev, act)

    def own_y(blk, act):
        whole(me, blk, OY, y_dev, act)

    def mates(blk, act):
        whole(xs, blk, PX, p_dev, act)
        whole(ys, blk, PY, p_dev, act)

    def cross(blk, ys_slot, xs_slot, act):
        fold = folded(blk)

        @pl.when(jnp.logical_and(blk < X_ONLY, fold))
        def _():
            act(rcopy(xs_slot, blk, FY, y_dev, PACK, Y_PACKED))
            act(rcopy(ys_slot, blk, FX, x_dev, PACK + Y_PACKED, RB - PACK - Y_PACKED))

        @pl.when(jnp.logical_and(blk < X_ONLY, jnp.logical_not(fold)))
        def _():
            act(rcopy(xs_slot, blk, FY, y_dev, 0, Y_ROWS))
            act(rcopy(ys_slot, blk, FX, x_dev, Y_ROWS, RB - Y_ROWS))

        @pl.when(blk >= X_ONLY)
        def _():
            whole(ys_slot, blk, FX, x_dev, act)

    def diag(blk, act):
        whole(ds, blk, PD, p_dev, act)

    start = lambda c: c.start()
    sent_out = lambda c: c.wait_send()
    landed = lambda c: c.wait_recv()

    def t_copy(slot, kind, dev):
        return pltpu.make_async_remote_copy(
            src_ref=t_buf.at[slot], dst_ref=t_buf.at[slot], send_sem=t_send.at[kind], recv_sem=t_recv.at[kind],
            device_id=dev, device_id_type=MESH)

    def local_v(n):
        k = GROUPS - n
        o = n * (n - 1) // 2
        return pltpu.make_async_copy(
            v_hbm.at[pl.ds(RB * k, RB * n), pl.ds(2 * PW * k, 2 * PW)],
            v_buf.at[me, pl.ds(RB * o, RB * n), :], loc_sem.at[n - 1])

    t_in = pltpu.make_async_copy(t_hbm, t_own, io_sem.at[0])
    z_in = pltpu.make_async_copy(z_hbm, x_buf, io_sem.at[1])
    soon = 4
    t_in.start()
    for n in range(1, soon + 1):
        local_v(n).start()

    barrier = pltpu.get_barrier_semaphore()
    for dev in (x_dev, y_dev, p_dev):
        pl.semaphore_signal(barrier, inc=1, device_id=dev, device_id_type=MESH)
    t_in.wait()
    for k in range(GROUPS):
        t_buf[col, k * PW:(k + 1) * PW, :] = jnp.concatenate(
            [t_own[2 * k * PW:(2 * k + 1) * PW, :], t_own[(2 * k + 1) * PW:(2 * k + 2) * PW, :]], axis=1)
    half_lane = lax.broadcasted_iota(jnp.int32, (PW, 128), 1) < PW

    def fold_own(n):
        r = RB * STARTS[n - 1]
        low = v_buf[me, r:r + PW, :]
        high = v_buf[me, r + PW:r + 2 * PW, :]
        v_buf[me, r + PW:r + 2 * PW, :] = jnp.where(half_lane, low, pltpu.roll(high, PW, 1))

    for n in range(1, soon + 1):
        local_v(n).wait()
        fold_own(n)
    for m in range(soon + 1, GROUPS + 1):
        local_v(m).start()
    z_in.start()
    pl.semaphore_wait(barrier, 3)

    for b in range(max(X_LEAD, Y_LEAD)):
        if b < X_LEAD:
            own_x(b, start)
        if b < Y_LEAD:
            own_y(b, start)
        if b == 1:
            t_copy(col, 0, x_dev).start()
            t_copy(col, 1, p_dev).start()
    for m in range(soon + 1, GROUPS + 1):
        local_v(m).wait()
        fold_own(m)
    z_in.wait()

    def pump(blk, _):
        whole(xs, blk, OX, x_dev, landed)
        whole(ys, blk, OY, y_dev, landed)
        cross(blk, ys, xs, start)
        mates(blk, start)

        @pl.when(blk + X_LEAD < BLOCKS)
        def _():
            own_x(blk + X_LEAD, start)

        @pl.when(blk + Y_LEAD < BLOCKS)
        def _():
            own_y(blk + Y_LEAD, start)
        return 0

    def pump_to(done, target):
        target = jnp.maximum(done, jnp.minimum(target, BLOCKS))
        lax.fori_loop(done, target, pump, 0)
        return target

    def take_diag(blk):
        cross(blk, ds, ds, landed)
        diag(blk, start)

    def need(blk):
        for kind in (OP, PX, PY, PD):
            whole(me, blk, kind, p_dev, landed)

    def unfold(t, fold):
        p = t[PW:2 * PW]
        top = jnp.concatenate(
            [jnp.where(half_lane, p, 0.0), jnp.where(half_lane, pltpu.roll(p, PW, 1), 0.0)], axis=0)
        return jnp.concatenate([jnp.where(fold, top, t[:2 * PW]), t[2 * PW:]], axis=0)

    def rows_of(blk, dds, fold):
        r = pl.ds(pl.multiple_of(blk * RB, RB), RB)
        return jnp.concatenate(
            [jnp.concatenate([unfold(v_buf[dd * 4 + e, r, :], fold) for e in range(4)], axis=1) for dd in dds], axis=0)

    def gram(cols, vals):
        first = [t[:HW] for t in cols]
        last = [t[HW:] for t in cols]
        vf = [v[:, :HW] for v in vals]
        vl = [v[:, HW:] for v in vals]
        return dot6(first, vf), dot6(first, vl), dot6(last, vl)

    lane = lax.broadcasted_iota(jnp.int32, (HW, 128), 1)
    lane_t = lax.broadcasted_iota(jnp.int32, (PW, 128), 1)
    zero_t = jnp.zeros((PW, 128), F32)

    def lanes_of(q, par):
        a, b = q[:, :128], q[:, 128:]
        if par == 0:
            return jnp.where(lane < PW, a, pltpu.roll(b, PW, 1))
        return jnp.where(lane < PW, pltpu.roll(a, PW, 1), b)

    def rows_par(q, par):
        return jnp.concatenate([q[par * PW:(par + 1) * PW], q[128 + par * PW:128 + (par + 1) * PW]], axis=0)

    def factors(k, par):
        tiles = []
        for e in range(4):
            t = t_buf[e, pl.ds(pl.multiple_of(k * PW, PW), PW), :]
            src = t if par == e % 2 else pltpu.roll(t, PW, 1)
            tiles.append(jnp.where(lane_t // PW == e % 2, src, 0.0))
        return tiles

    def diag256(tiles):
        return jnp.concatenate(
            [jnp.concatenate([t, zero_t] if e < 2 else [zero_t, t], axis=1) for e, t in enumerate(tiles)], axis=0)

    def merge(tiles, gaa, gab, gbb):
        whole = diag256(tiles)
        u = jnp.concatenate([jnp.where(lane_t < PW, 0.0, gaa[:PW]), jnp.where(lane_t < PW, 0.0, gbb[:PW])], axis=1)
        c = dot_f32(u, whole)
        rhs = jnp.concatenate([
            jnp.concatenate([c[:, :128], zero_t], axis=1), jnp.zeros((PW, HW), F32),
            jnp.concatenate([zero_t, c[:, 128:]], axis=1), jnp.zeros((PW, HW), F32)], axis=0)
        lhs = jnp.concatenate([tiles[0] + tiles[1], tiles[2] + tiles[3]], axis=1)
        p = dot_f32(lhs, rhs)
        ta = jnp.concatenate([tiles[0] - p[:, :128], tiles[1]], axis=0)
        tb = jnp.concatenate([tiles[2] - p[:, 128:], tiles[3]], axis=0)
        tab = dot_f32(ta, dot_f32(gab, tb))
        return jnp.concatenate([
            jnp.concatenate([ta, -tab], axis=1), jnp.concatenate([jnp.zeros_like(tb), tb], axis=1)], axis=0)

    def g_copy(n):
        return pltpu.make_async_remote_copy(
            src_ref=g_part, dst_ref=g_in.at[lax.rem(n, 2)], send_sem=g_send, recv_sem=g_recv.at[lax.rem(n, 2)],
            device_id=p_dev, device_id_type=MESH)

    def group(step, carry):
        pumped, diag_done = carry
        n = step + 1
        k = GROUPS - n
        first = n * step // 2
        w_buf[...] = jnp.zeros_like(w_buf)

        @pl.when(n > 2)
        def _():
            g_copy(n - 1).wait_send()
        g_part[...] = jnp.zeros_like(g_part)

        def arrive(i, carry, pumping=True):
            pumped, diag_done = carry
            blk = first + i
            if pumping:
                pumped = pump_to(pumped, blk + AHEAD_W)

            def dg(b, _):
                take_diag(b)
                return 0
            diag_to = jnp.minimum(blk + 2, BLOCKS)
            lax.fori_loop(diag_done, diag_to, dg, 0)
            need(blk)
            return pumped, diag_to

        def load(i):
            r = pl.ds(pl.multiple_of((k + i) * RB, RB), RB)
            v = split3(rows_of(first + i, (core, 1 - core), i == 0))
            x = split3(jnp.concatenate([x_buf[core, r, :], x_buf[1 - core, r, :]], axis=0))
            t = [p.T for p in v]
            w_buf[...] += dot6(t, x)
            return v, t

        def gather_step(i, carry):
            carry = arrive(i, carry, False)
            v, t = load(i)
            gs = gram([p[:, :RB] for p in t], [p[:RB] for p in v])
            for q in range(3):
                g_part[q] += gs[q]
            pumped, diag_done = carry
            return pump_to(pumped, first + i + 1 + AHEAD_W), diag_done

        carry = lax.fori_loop(0, step, gather_step, (pumped, diag_done))
        pumped, diag_done = arrive(step, carry)

        @pl.when(step > 0)
        def _():
            g_copy(n).start()
        v, t = load(step)
        gs = gram(t, v)
        for q in range(3):
            g_last[q] = gs[q]

        @pl.when(step == 0)
        def _():
            t_copy(xcol, 0, x_dev).wait_recv()
            t_copy(xcol, 2, p_dev).start()
            t_copy(pcol, 1, p_dev).wait_recv()
            t_copy(lax.rem(pcol + 2, 4), 2, p_dev).wait_recv()

        @pl.when(step > 0)
        def _():
            g_copy(n).wait_recv()
            for q in range(3):
                g_last[q] += g_part[q] + g_in[lax.rem(n, 2), q]
        lanes = [[lanes_of(g_last[q], par) for par in range(2)] for q in range(3)]
        ts = [merge(factors(k, par), *[rows_par(lanes[q][par], par) for q in range(3)]) for par in range(2)]
        g01 = jnp.concatenate([
            jnp.concatenate([rows_par(lanes[0][1], 0), rows_par(lanes[1][1], 0)], axis=1),
            jnp.concatenate([rows_par(lanes[1][0], 1).T, rows_par(lanes[2][1], 0)], axis=1)], axis=0)
        w0, w1 = [jnp.concatenate([w_buf[e * 128 + par * PW:e * 128 + (par + 1) * PW, :] for e in range(4)], axis=0)
                  for par in range(2)]
        y1 = dot_f32(ts[1], w1)
        y0 = dot_f32(ts[0], w0 - dot_f32(g01, y1))
        @pl.when(k == 0)
        def _():
            for e in range(4):
                for par, y in enumerate((y0, y1)):
                    y_out[e * 128 + par * PW:e * 128 + (par + 1) * PW, :] = y[e * PW:(e + 1) * PW]
        for e in range(4):
            for par, y in enumerate((y0, y1)):
                for q, part in enumerate(split3(y[e * PW:(e + 1) * PW])):
                    y_buf[q, e * 128 + par * PW:e * 128 + (par + 1) * PW, :] = part

        def update_step(i, pumped):
            blk = first + i
            pumped = pump_to(pumped, first + n - 1 + AHEAD_W + (i + 1) // 2)
            rx = pl.ds(pl.multiple_of((k + i) * RB, RB), RB)
            delta = dot6(split3(rows_of(blk, (0, 1), i == 0)), [y_buf[q] for q in range(3)])
            x_buf[0, rx, :] = x_buf[0, rx, :] - delta[:RB]
            x_buf[1, rx, :] = x_buf[1, rx, :] - delta[RB:]

            @pl.when(jnp.logical_and(k == 1, i < GROUPS - LAST_GIVES))
            def _():
                give(i).start()
            return pumped

        pumped = lax.fori_loop(0, jnp.where(k == 0, 0, n), update_step, pumped)
        return pumped, diag_done

    def give(i):
        r = pl.ds(pl.multiple_of(i * RB, RB), RB)
        return pltpu.make_async_remote_copy(
            src_ref=x_buf.at[orow, r, :], dst_ref=xb_buf.at[r, :], send_sem=c_send.at[i], recv_sem=c_recv.at[i],
            device_id=y_dev, device_id_type=MESH)

    y_copy = pltpu.make_async_remote_copy(
        src_ref=y_out, dst_ref=y_in, send_sem=y_send, recv_sem=y_recv, device_id=y_dev, device_id_type=MESH)

    lax.fori_loop(0, GROUPS, group, (0, 0))

    first_last = BLOCKS - GROUPS

    def span_of(i):
        return pl.ds(pl.multiple_of(i * SPAN, SPAN), SPAN)

    def v_span(i):
        r = pl.ds(pl.multiple_of(first_last * RB + i * SPAN, SPAN), SPAN)
        return split3(jnp.concatenate([unfold(v_buf[row * 4 + e, r, :], i == 0) for e in range(4)], axis=1))

    def half_of(i, at):
        return out_ref.at[span_of(i), pl.ds(pl.multiple_of(at * COLS, COLS), COLS)]

    spans = ROWS // SPAN

    def mine(i, _):
        half_of(i, row)[...] = x_buf[row, span_of(i), :] - dot6(v_span(i), [y_buf[q] for q in range(3)])

        @pl.when(i == 0)
        def _():
            y_copy.start()
            for g in range(GROUPS - LAST_GIVES, GROUPS):
                give(g).start()
        return 0
    lax.fori_loop(0, spans, mine, 0)

    y_copy.wait_recv()
    for q, part in enumerate(split3(y_in[...])):
        yb_buf[q] = part

    def theirs(i, _):
        for h in range(SPAN // RB):
            give(i * (SPAN // RB) + h).wait_recv()
        half_of(i, orow)[...] = xb_buf[span_of(i), :] - dot6(v_span(i), [yb_buf[q] for q in range(3)])
        return 0
    lax.fori_loop(0, spans, theirs, 0)

    def drain(blk, _):
        own_x(blk, sent_out)
        own_y(blk, sent_out)
        cross(blk, ys, xs, sent_out)
        mates(blk, sent_out)
        diag(blk, sent_out)
        return 0
    lax.fori_loop(0, BLOCKS, drain, 0)
    t_copy(col, 0, x_dev).wait_send()
    t_copy(col, 1, p_dev).wait_send()
    t_copy(xcol, 2, p_dev).wait_send()
    g_copy(GROUPS).wait_send()


    y_copy.wait_send()

    def drain_c(i, _):
        give(i).wait_send()
        return 0
    lax.fori_loop(0, GROUPS, drain_c, 0)


def solution(mesh):
    def local_apply(v_loc, t_loc, z_loc):
        t_pk = t_loc.reshape(2 * GROUPS * PW, PW)
        z_pk = z_loc.reshape(2, ROWS, COLS)
        any_spec = pl.BlockSpec(memory_space=pl.ANY)
        return pl.pallas_call(
            kernel,
            out_shape=pltpu.VMEM((ROWS, 2 * COLS), F32),
            in_specs=[any_spec] * 3,
            out_specs=pl.BlockSpec(memory_space=pltpu.VMEM),
            scratch_shapes=[
                pltpu.VMEM((8, BLOCKS * RB, 128), F32),
                pltpu.VMEM((2 * GROUPS * PW, PW), F32),
                pltpu.VMEM((4, GROUPS * PW, 2 * PW), F32),
                pltpu.VMEM((2, ROWS, COLS), F32),
                pltpu.VMEM((GW, COLS), F32),
                pltpu.VMEM((3, HW, HW), F32),
                pltpu.VMEM((2, 3, HW, HW), F32),
                pltpu.VMEM((3, HW, HW), F32),
                pltpu.VMEM((3, GW, COLS), BF16),
                pltpu.VMEM((ROWS, COLS), F32),
                pltpu.VMEM((GW, COLS), F32),
                pltpu.VMEM((GW, COLS), F32),
                pltpu.VMEM((3, GW, COLS), BF16),
                pltpu.SemaphoreType.DMA((GROUPS,)),
                pltpu.SemaphoreType.DMA((3,)),
                pltpu.SemaphoreType.DMA((3,)),
                pltpu.SemaphoreType.DMA((8, BLOCKS)),
                pltpu.SemaphoreType.DMA((8, BLOCKS)),
                pltpu.SemaphoreType.DMA,
                pltpu.SemaphoreType.DMA((2,)),
                pltpu.SemaphoreType.DMA((GROUPS,)),
                pltpu.SemaphoreType.DMA((GROUPS,)),
                pltpu.SemaphoreType.DMA,
                pltpu.SemaphoreType.DMA,
                pltpu.SemaphoreType.DMA((2,)),
            ],
            compiler_params=pltpu.CompilerParams(
                collective_id=0, has_side_effects=True, vmem_limit_bytes=VMEM_LIMIT),
            name='panels',
        )(v_loc, t_pk, z_pk)

    return jax.shard_map(local_apply, mesh=mesh,
                         in_specs=(P('row', 'col'), P('col', None, None), P(None, ('col', 'row'))),
                         out_specs=P('row', 'col'), check_vma=False)
```

```python
import jax
import jax.numpy as jnp
from jax import lax
from jax.experimental import pallas as pl
from jax.experimental.pallas import tpu as pltpu
from jax.sharding import PartitionSpec as P

F32 = jnp.float32
BF16 = jnp.bfloat16
MESH = pl.DeviceIdType.MESH
PW = 64
RB = 256
GROUPS = 8
BLOCKS = GROUPS * (GROUPS + 1) // 2
PACK = 64
STARTS = [n * (n - 1) // 2 for n in range(1, GROUPS + 1)]
Y_ROWS = 128
Y_PACKED = 96
X_ONLY = 30
LAST_GIVES = 2
SPAN = RB
AHEAD_W = 5
X_LEAD = 4
Y_LEAD = 6
COLS = 256
ROWS = 2048
GW = GROUPS * PW
HW = GW // 2
VMEM_LIMIT = 60 * 10**6


def split3(x):
    a = x.astype(BF16)
    r = x - a.astype(F32)
    b = r.astype(BF16)
    c = (r - b.astype(F32)).astype(BF16)
    return a, b, c


def dot6(lhs, rhs):
    a1, a2, a3 = lhs
    b1, b2, b3 = rhs

    def mm(p, q):
        return jnp.dot(p, q, preferred_element_type=F32)

    return ((mm(a3, b1) + mm(a1, b3)) + mm(a2, b2)) + (mm(a2, b1) + mm(a1, b2)) + mm(a1, b1)


def dot_f32(a, b):
    return dot6(split3(a), split3(b))


def kernel(v_hbm, t_hbm, z_hbm, out_ref, v_buf, t_own, t_buf, x_buf, w_buf, g_part, g_in, g_last, y_buf,
           xb_buf, y_out, y_in, yb_buf, loc_sem, t_send, t_recv, send, recv, g_send, g_recv, c_send, c_recv,
           y_send, y_recv, io_sem):
    row = lax.axis_index('row')
    col = lax.axis_index('col')
    orow = 1 - row
    xcol = lax.rem(col + 2, 4)
    core = lax.rem(col, 2)
    pcol = col + 1 - 2 * core
    x_dev, y_dev, p_dev = (row, xcol), (orow, col), (row, pcol)
    me = row * 4 + col
    xs = row * 4 + xcol
    ys = orow * 4 + col
    ds = orow * 4 + xcol

    def vmem(slot, blk, off=0, size=RB):
        return v_buf.at[slot, pl.ds(pl.multiple_of(blk * RB + off, 8), size), :]

    def rcopy(slot, blk, kind, dev, off=0, size=RB):
        return pltpu.make_async_remote_copy(
            src_ref=vmem(slot, blk, off, size), dst_ref=vmem(slot, blk, off, size),
            send_sem=send.at[kind, blk], recv_sem=recv.at[kind, blk], device_id=dev, device_id_type=MESH)

    OX, OY, OP, FX, FY, PX, PY, PD = range(8)

    def folded(blk):
        found = blk == STARTS[0]
        for b in STARTS[1:]:
            found = jnp.logical_or(found, blk == b)
        return found

    def whole(slot, blk, kind, dev, act):
        if isinstance(blk, int):
            off = PACK if blk in STARTS else 0
            act(rcopy(slot, blk, kind, dev, off, RB - off))
            return
        fold = folded(blk)

        @pl.when(fold)
        def _():
            act(rcopy(slot, blk, kind, dev, PACK, RB - PACK))

        @pl.when(jnp.logical_not(fold))
        def _():
            act(rcopy(slot, blk, kind, dev))

    def own_x(blk, act):
        whole(me, blk, OX, x_dev, act)
        whole(me, blk, OP, p_dev, act)

    def own_y(blk, act):
        whole(me, blk, OY, y_dev, act)

    def mates(blk, act):
        whole(xs, blk, PX, p_dev, act)
        whole(ys, blk, PY, p_dev, act)

    def cross(blk, ys_slot, xs_slot, act):
        fold = folded(blk)

        @pl.when(jnp.logical_and(blk < X_ONLY, fold))
        def _():
            act(rcopy(xs_slot, blk, FY, y_dev, PACK, Y_PACKED))
            act(rcopy(ys_slot, blk, FX, x_dev, PACK + Y_PACKED, RB - PACK - Y_PACKED))

        @pl.when(jnp.logical_and(blk < X_ONLY, jnp.logical_not(fold)))
        def _():
            act(rcopy(xs_slot, blk, FY, y_dev, 0, Y_ROWS))
            act(rcopy(ys_slot, blk, FX, x_dev, Y_ROWS, RB - Y_ROWS))

        @pl.when(blk >= X_ONLY)
        def _():
            whole(ys_slot, blk, FX, x_dev, act)

    def diag(blk, act):
        whole(ds, blk, PD, p_dev, act)

    start = lambda c: c.start()
    sent_out = lambda c: c.wait_send()
    landed = lambda c: c.wait_recv()

    def t_copy(slot, kind, dev):
        return pltpu.make_async_remote_copy(
            src_ref=t_buf.at[slot], dst_ref=t_buf.at[slot], send_sem=t_send.at[kind], recv_sem=t_recv.at[kind],
            device_id=dev, device_id_type=MESH)

    def local_v(n):
        k = GROUPS - n
        o = n * (n - 1) // 2
        return pltpu.make_async_copy(
            v_hbm.at[pl.ds(RB * k, RB * n), pl.ds(2 * PW * k, 2 * PW)],
            v_buf.at[me, pl.ds(RB * o, RB * n), :], loc_sem.at[n - 1])

    t_in = pltpu.make_async_copy(t_hbm, t_own, io_sem.at[0])
    z_in = pltpu.make_async_copy(z_hbm, x_buf, io_sem.at[1])
    soon = 4
    t_in.start()
    for n in range(1, soon + 1):
        local_v(n).start()

    barrier = pltpu.get_barrier_semaphore()
    for dev in (x_dev, y_dev, p_dev):
        pl.semaphore_signal(barrier, inc=1, device_id=dev, device_id_type=MESH)
    t_in.wait()
    for k in range(GROUPS):
        t_buf[col, k * PW:(k + 1) * PW, :] = jnp.concatenate(
            [t_own[2 * k * PW:(2 * k + 1) * PW, :], t_own[(2 * k + 1) * PW:(2 * k + 2) * PW, :]], axis=1)
    half_lane = lax.broadcasted_iota(jnp.int32, (PW, 128), 1) < PW

    def fold_own(n):
        r = RB * STARTS[n - 1]
        low = v_buf[me, r:r + PW, :]
        high = v_buf[me, r + PW:r + 2 * PW, :]
        v_buf[me, r + PW:r + 2 * PW, :] = jnp.where(half_lane, low, pltpu.roll(high, PW, 1))

    for n in range(1, soon + 1):
        local_v(n).wait()
        fold_own(n)
    for m in range(soon + 1, GROUPS + 1):
        local_v(m).start()
    z_in.start()
    pl.semaphore_wait(barrier, 3)

    for b in range(max(X_LEAD, Y_LEAD)):
        if b < X_LEAD:
            own_x(b, start)
        if b < Y_LEAD:
            own_y(b, start)
        if b == 3:
            t_copy(col, 0, x_dev).start()
            t_copy(col, 1, p_dev).start()
    for m in range(soon + 1, GROUPS + 1):
        local_v(m).wait()
        fold_own(m)
    z_in.wait()

    def pump(blk, _):
        whole(xs, blk, OX, x_dev, landed)
        whole(ys, blk, OY, y_dev, landed)
        cross(blk, ys, xs, start)
        mates(blk, start)

        @pl.when(blk + X_LEAD < BLOCKS)
        def _():
            own_x(blk + X_LEAD, start)

        @pl.when(blk + Y_LEAD < BLOCKS)
        def _():
            own_y(blk + Y_LEAD, start)
        return 0

    def pump_to(done, target):
        target = jnp.maximum(done, jnp.minimum(target, BLOCKS))
        lax.fori_loop(done, target, pump, 0)
        return target

    def take_diag(blk):
        cross(blk, ds, ds, landed)
        diag(blk, start)

    def need(blk):
        for kind in (OP, PX, PY, PD):
            whole(me, blk, kind, p_dev, landed)

    def unfold(t, fold):
        p = t[PW:2 * PW]
        top = jnp.concatenate(
            [jnp.where(half_lane, p, 0.0), jnp.where(half_lane, pltpu.roll(p, PW, 1), 0.0)], axis=0)
        return jnp.concatenate([jnp.where(fold, top, t[:2 * PW]), t[2 * PW:]], axis=0)

    def rows_of(blk, dds, fold):
        r = pl.ds(pl.multiple_of(blk * RB, RB), RB)
        return jnp.concatenate(
            [jnp.concatenate([unfold(v_buf[dd * 4 + e, r, :], fold) for e in range(4)], axis=1) for dd in dds], axis=0)

    def gram(cols, vals):
        first = [t[:HW] for t in cols]
        last = [t[HW:] for t in cols]
        vf = [v[:, :HW] for v in vals]
        vl = [v[:, HW:] for v in vals]
        return dot6(first, vf), dot6(first, vl), dot6(last, vl)

    lane = lax.broadcasted_iota(jnp.int32, (HW, 128), 1)
    lane_t = lax.broadcasted_iota(jnp.int32, (PW, 128), 1)
    zero_t = jnp.zeros((PW, 128), F32)

    def lanes_of(q, par):
        a, b = q[:, :128], q[:, 128:]
        if par == 0:
            return jnp.where(lane < PW, a, pltpu.roll(b, PW, 1))
        return jnp.where(lane < PW, pltpu.roll(a, PW, 1), b)

    def rows_par(q, par):
        return jnp.concatenate([q[par * PW:(par + 1) * PW], q[128 + par * PW:128 + (par + 1) * PW]], axis=0)

    def factors(k, par):
        tiles = []
        for e in range(4):
            t = t_buf[e, pl.ds(pl.multiple_of(k * PW, PW), PW), :]
            src = t if par == e % 2 else pltpu.roll(t, PW, 1)
            tiles.append(jnp.where(lane_t // PW == e % 2, src, 0.0))
        return tiles

    def diag256(tiles):
        return jnp.concatenate(
            [jnp.concatenate([t, zero_t] if e < 2 else [zero_t, t], axis=1) for e, t in enumerate(tiles)], axis=0)

    def merge(tiles, gaa, gab, gbb):
        whole = diag256(tiles)
        u = jnp.concatenate([jnp.where(lane_t < PW, 0.0, gaa[:PW]), jnp.where(lane_t < PW, 0.0, gbb[:PW])], axis=1)
        c = dot_f32(u, whole)
        rhs = jnp.concatenate([
            jnp.concatenate([c[:, :128], zero_t], axis=1), jnp.zeros((PW, HW), F32),
            jnp.concatenate([zero_t, c[:, 128:]], axis=1), jnp.zeros((PW, HW), F32)], axis=0)
        lhs = jnp.concatenate([tiles[0] + tiles[1], tiles[2] + tiles[3]], axis=1)
        p = dot_f32(lhs, rhs)
        ta = jnp.concatenate([tiles[0] - p[:, :128], tiles[1]], axis=0)
        tb = jnp.concatenate([tiles[2] - p[:, 128:], tiles[3]], axis=0)
        tab = dot_f32(ta, dot_f32(gab, tb))
        return jnp.concatenate([
            jnp.concatenate([ta, -tab], axis=1), jnp.concatenate([jnp.zeros_like(tb), tb], axis=1)], axis=0)

    def g_copy(n):
        return pltpu.make_async_remote_copy(
            src_ref=g_part, dst_ref=g_in.at[lax.rem(n, 2)], send_sem=g_send, recv_sem=g_recv.at[lax.rem(n, 2)],
            device_id=p_dev, device_id_type=MESH)

    def group(step, carry):
        pumped, diag_done = carry
        n = step + 1
        k = GROUPS - n
        first = n * step // 2
        w_buf[...] = jnp.zeros_like(w_buf)

        @pl.when(n > 2)
        def _():
            g_copy(n - 1).wait_send()
        g_part[...] = jnp.zeros_like(g_part)

        def arrive(i, carry, pumping=True):
            pumped, diag_done = carry
            blk = first + i
            if pumping:
                pumped = pump_to(pumped, blk + AHEAD_W)

            def dg(b, _):
                take_diag(b)
                return 0
            diag_to = jnp.minimum(blk + 2, BLOCKS)
            lax.fori_loop(diag_done, diag_to, dg, 0)
            need(blk)
            return pumped, diag_to

        def load(i):
            r = pl.ds(pl.multiple_of((k + i) * RB, RB), RB)
            v = split3(rows_of(first + i, (core, 1 - core), i == 0))
            x = split3(jnp.concatenate([x_buf[core, r, :], x_buf[1 - core, r, :]], axis=0))
            t = [p.T for p in v]
            w_buf[...] += dot6(t, x)
            return v, t

        def gather_step(i, carry):
            carry = arrive(i, carry, False)
            v, t = load(i)
            gs = gram([p[:, :RB] for p in t], [p[:RB] for p in v])
            for q in range(3):
                g_part[q] += gs[q]
            pumped, diag_done = carry
            return pump_to(pumped, first + i + 1 + AHEAD_W), diag_done

        carry = lax.fori_loop(0, step, gather_step, (pumped, diag_done))
        pumped, diag_done = arrive(step, carry)

        @pl.when(step > 0)
        def _():
            g_copy(n).start()
        v, t = load(step)
        gs = gram(t, v)
        for q in range(3):
            g_last[q] = gs[q]

        @pl.when(step == 0)
        def _():
            t_copy(xcol, 0, x_dev).wait_recv()
            t_copy(xcol, 2, p_dev).start()
            t_copy(pcol, 1, p_dev).wait_recv()
            t_copy(lax.rem(pcol + 2, 4), 2, p_dev).wait_recv()

        @pl.when(step > 0)
        def _():
            g_copy(n).wait_recv()
            for q in range(3):
                g_last[q] += g_part[q] + g_in[lax.rem(n, 2), q]
        lanes = [[lanes_of(g_last[q], par) for par in range(2)] for q in range(3)]
        ts = [merge(factors(k, par), *[rows_par(lanes[q][par], par) for q in range(3)]) for par in range(2)]
        g01 = jnp.concatenate([
            jnp.concatenate([rows_par(lanes[0][1], 0), rows_par(lanes[1][1], 0)], axis=1),
            jnp.concatenate([rows_par(lanes[1][0], 1).T, rows_par(lanes[2][1], 0)], axis=1)], axis=0)
        w0, w1 = [jnp.concatenate([w_buf[e * 128 + par * PW:e * 128 + (par + 1) * PW, :] for e in range(4)], axis=0)
                  for par in range(2)]
        y1 = dot_f32(ts[1], w1)
        y0 = dot_f32(ts[0], w0 - dot_f32(g01, y1))
        @pl.when(k == 0)
        def _():
            for e in range(4):
                for par, y in enumerate((y0, y1)):
                    y_out[e * 128 + par * PW:e * 128 + (par + 1) * PW, :] = y[e * PW:(e + 1) * PW]
        for e in range(4):
            for par, y in enumerate((y0, y1)):
                for q, part in enumerate(split3(y[e * PW:(e + 1) * PW])):
                    y_buf[q, e * 128 + par * PW:e * 128 + (par + 1) * PW, :] = part

        def update_step(i, pumped):
            blk = first + i
            pumped = pump_to(pumped, first + n - 1 + AHEAD_W + (i + 1) // 2)
            rx = pl.ds(pl.multiple_of((k + i) * RB, RB), RB)
            delta = dot6(split3(rows_of(blk, (0, 1), i == 0)), [y_buf[q] for q in range(3)])
            x_buf[0, rx, :] = x_buf[0, rx, :] - delta[:RB]
            x_buf[1, rx, :] = x_buf[1, rx, :] - delta[RB:]

            @pl.when(jnp.logical_and(k == 1, i < GROUPS - LAST_GIVES))
            def _():
                give(i).start()
            return pumped

        pumped = lax.fori_loop(0, jnp.where(k == 0, 0, n), update_step, pumped)
        return pumped, diag_done

    def give(i):
        r = pl.ds(pl.multiple_of(i * RB, RB), RB)
        return pltpu.make_async_remote_copy(
            src_ref=x_buf.at[orow, r, :], dst_ref=xb_buf.at[r, :], send_sem=c_send.at[i], recv_sem=c_recv.at[i],
            device_id=y_dev, device_id_type=MESH)

    y_copy = pltpu.make_async_remote_copy(
        src_ref=y_out, dst_ref=y_in, send_sem=y_send, recv_sem=y_recv, device_id=y_dev, device_id_type=MESH)

    lax.fori_loop(0, GROUPS, group, (0, 0))

    first_last = BLOCKS - GROUPS

    def span_of(i):
        return pl.ds(pl.multiple_of(i * SPAN, SPAN), SPAN)

    def v_span(i):
        r = pl.ds(pl.multiple_of(first_last * RB + i * SPAN, SPAN), SPAN)
        return split3(jnp.concatenate([unfold(v_buf[row * 4 + e, r, :], i == 0) for e in range(4)], axis=1))

    def half_of(i, at):
        return out_ref.at[span_of(i), pl.ds(pl.multiple_of(at * COLS, COLS), COLS)]

    spans = ROWS // SPAN

    def mine(i, _):
        half_of(i, row)[...] = x_buf[row, span_of(i), :] - dot6(v_span(i), [y_buf[q] for q in range(3)])

        @pl.when(i == 0)
        def _():
            y_copy.start()
            for g in range(GROUPS - LAST_GIVES, GROUPS):
                give(g).start()
        return 0
    lax.fori_loop(0, spans, mine, 0)

    y_copy.wait_recv()
    for q, part in enumerate(split3(y_in[...])):
        yb_buf[q] = part

    def theirs(i, _):
        for h in range(SPAN // RB):
            give(i * (SPAN // RB) + h).wait_recv()
        half_of(i, orow)[...] = xb_buf[span_of(i), :] - dot6(v_span(i), [yb_buf[q] for q in range(3)])
        return 0
    lax.fori_loop(0, spans, theirs, 0)

    def drain(blk, _):
        own_x(blk, sent_out)
        own_y(blk, sent_out)
        cross(blk, ys, xs, sent_out)
        mates(blk, sent_out)
        diag(blk, sent_out)
        return 0
    lax.fori_loop(0, BLOCKS, drain, 0)
    t_copy(col, 0, x_dev).wait_send()
    t_copy(col, 1, p_dev).wait_send()
    t_copy(xcol, 2, p_dev).wait_send()
    g_copy(GROUPS).wait_send()


    y_copy.wait_send()

    def drain_c(i, _):
        give(i).wait_send()
        return 0
    lax.fori_loop(0, GROUPS, drain_c, 0)


def solution(mesh):
    def local_apply(v_loc, t_loc, z_loc):
        t_pk = t_loc.reshape(2 * GROUPS * PW, PW)
        z_pk = z_loc.reshape(2, ROWS, COLS)
        any_spec = pl.BlockSpec(memory_space=pl.ANY)
        return pl.pallas_call(
            kernel,
            out_shape=pltpu.VMEM((ROWS, 2 * COLS), F32),
            in_specs=[any_spec] * 3,
            out_specs=pl.BlockSpec(memory_space=pltpu.VMEM),
            scratch_shapes=[
                pltpu.VMEM((8, BLOCKS * RB, 128), F32),
                pltpu.VMEM((2 * GROUPS * PW, PW), F32),
                pltpu.VMEM((4, GROUPS * PW, 2 * PW), F32),
                pltpu.VMEM((2, ROWS, COLS), F32),
                pltpu.VMEM((GW, COLS), F32),
                pltpu.VMEM((3, HW, HW), F32),
                pltpu.VMEM((2, 3, HW, HW), F32),
                pltpu.VMEM((3, HW, HW), F32),
                pltpu.VMEM((3, GW, COLS), BF16),
                pltpu.VMEM((ROWS, COLS), F32),
                pltpu.VMEM((GW, COLS), F32),
                pltpu.VMEM((GW, COLS), F32),
                pltpu.VMEM((3, GW, COLS), BF16),
                pltpu.SemaphoreType.DMA((GROUPS,)),
                pltpu.SemaphoreType.DMA((3,)),
                pltpu.SemaphoreType.DMA((3,)),
                pltpu.SemaphoreType.DMA((8, BLOCKS)),
                pltpu.SemaphoreType.DMA((8, BLOCKS)),
                pltpu.SemaphoreType.DMA,
                pltpu.SemaphoreType.DMA((2,)),
                pltpu.SemaphoreType.DMA((GROUPS,)),
                pltpu.SemaphoreType.DMA((GROUPS,)),
                pltpu.SemaphoreType.DMA,
                pltpu.SemaphoreType.DMA,
                pltpu.SemaphoreType.DMA((2,)),
            ],
            compiler_params=pltpu.CompilerParams(
                collective_id=0, has_side_effects=True, vmem_limit_bytes=VMEM_LIMIT),
            name='panels',
        )(v_loc, t_pk, z_pk)

    return jax.shard_map(local_apply, mesh=mesh,
                         in_specs=(P('row', 'col'), P('col', None, None), P(None, ('col', 'row'))),
                         out_specs=P('row', 'col'), check_vma=False)
```
